32 devices in a mesh: srv: 16 (over z, y, x), grp: 2 (over core).
Axes of the slice: x: 2, y: 2, z: 4, core: 2. Of those that a mesh axis runs over, the one named last changes fastest.
Arguments:
- basis_modes: float32 [64, 64, 3072], P(None, ('srv', 'grp')), may hold values from -10 to 10
- weights: float32 [64], replicated, may hold values from 0.5 to 4
- snapshots: float32 [16, 64, 3072], P(None, 'srv', 'grp'), may hold values from -10 to 10
Outputs:
- new_modes: float32 [80, 64, 3072], P(None, ('srv', 'grp'))
- factor: float32 [80, 80], replicated
The draws below stay inside these ranges and needn't reach their ends.
All inputs are finite; a program needn't handle non-finite values.
Results may differ from the reference program's by a relative error of at most 0.00009.
Values sent between devices are 32-bit elements; how exact they have to be, the bound alone decides.
No kernel may reach another device: no remote copies, remote signals or barrier semaphores. Data moves between devices by JAX's collectives and lax.ppermute only.
A program may use at most 64 MiB of HBM per device.

```python
import math
import jax
import jax.numpy as jnp
from jax import lax

MODES = 64
SNAPS = 16
COLS = 3072
ROWS = 64
PANEL = 80


def shared_fields(key):
    base = jax.random.fold_in(key, 31)
    key_field, key_mixing, key_coupling, key_noise = jax.random.split(base, 4)
    field = jax.random.truncated_normal(key_field, -4.0, 4.0, (MODES, ROWS * COLS), jnp.float32)
    mixing = jnp.eye(MODES, dtype=jnp.float32) + 0.5 * MODES ** (-0.5) * jax.random.truncated_normal(key_mixing, -3.0, 3.0, (MODES, MODES), jnp.float32)
    mixed = jnp.dot(mixing, field, precision=lax.Precision.HIGHEST)
    position = jnp.arange(ROWS, dtype=jnp.float32) / max(ROWS - 1, 1)
    power = 1.0 + 2.0 * position
    noise = 0.6 * jax.random.truncated_normal(key_noise, -4.0, 4.0, (SNAPS, ROWS * COLS), jnp.float32)
    amplitude = jnp.repeat(jnp.sqrt(power), COLS)
    coupling = MODES ** (-0.5) * jax.random.truncated_normal(key_coupling, -3.0, 3.0, (SNAPS, MODES), jnp.float32)
    basis = jnp.clip(amplitude * mixed, -10.0, 10.0)
    fresh = jnp.clip(amplitude * (jnp.dot(coupling, mixed, precision=lax.Precision.HIGHEST) + noise), -10.0, 10.0)
    return (basis.reshape(MODES, ROWS, COLS), fresh.reshape(SNAPS, ROWS, COLS))


def draw_basis_modes(key, part):
    return shared_fields(key)[0]


def draw_snapshots(key, part):
    return shared_fields(key)[1]


def setup_inputs(seed: int = 0) -> dict:
    key_of = jax.random.split(jax.random.key(seed), 4)
    basis_modes = draw_basis_modes(jax.random.fold_in(key_of[3], 71), 0)
    weights = jnp.clip(jnp.exp(jax.random.uniform(key_of[1], (MODES,), jnp.float32, math.log(0.5), math.log(4.0))), 0.5, 4.0)
    snapshots = draw_snapshots(jax.random.fold_in(key_of[3], 71), 0)
    return dict(basis_modes=basis_modes, weights=weights, snapshots=snapshots)


def reference(basis_modes, weights, snapshots):
    scaled = basis_modes * weights[:, None, None]
    panel = jnp.concatenate([scaled, snapshots], axis=0).reshape(PANEL, ROWS * COLS)
    gram = jnp.dot(panel.astype(jnp.float32), panel.T.astype(jnp.float32), precision=lax.Precision.HIGHEST, preferred_element_type=jnp.float32) / (ROWS * COLS)
    factor = jnp.linalg.cholesky(gram)
    inverse = lax.linalg.triangular_solve(factor, jnp.eye(PANEL, dtype=jnp.float32), left_side=True, lower=True)
    result = jnp.dot(inverse.astype(jnp.float32), panel.astype(jnp.float32), precision=lax.Precision.HIGHEST, preferred_element_type=jnp.float32)
    return (result.reshape(PANEL, ROWS, COLS), factor)
```

```python
import jax
import jax.numpy as jnp
from jax import lax
from jax.sharding import PartitionSpec as P

MODES = 64
SNAPS = 16


AXES = ("srv", "grp")


def total(value):
    servers, cores = lax.axis_size("srv"), lax.axis_size("grp")
    if servers & (servers - 1) or cores != 2:
        return lax.psum(value, AXES)
    count = servers * cores
    masks = [1] + [2 * bit + 1 for bit in (1 << p for p in range(servers.bit_length() - 1))]
    for mask in masks:
        value = value + lax.ppermute(value, AXES, [(i, i ^ mask) for i in range(count)])
    return value


def merged_factor(local_gram):
    return jnp.linalg.cholesky(total(local_gram))


def per_device(basis_modes, weights, snapshots):
    width = MODES + SNAPS
    total_cells = (
        basis_modes.shape[1] * basis_modes.shape[2] * lax.axis_size("srv") * lax.axis_size("grp")
    )
    scaled = basis_modes * weights[:, None, None]
    arrived = lax.all_to_all(snapshots, "grp", split_axis=1, concat_axis=2, tiled=True)
    panel = jnp.concatenate([scaled, arrived], axis=0).reshape(width, -1)
    local_gram = (
        jnp.dot(panel, panel.T, precision=lax.Precision.HIGHEST, preferred_element_type=jnp.float32)
        / total_cells
    )
    factor = merged_factor(local_gram)
    inverse = lax.linalg.triangular_solve(
        factor, jnp.eye(width, dtype=jnp.float32), left_side=True, lower=True
    )
    result = jnp.dot(
        inverse, panel, precision=lax.Precision.HIGHEST, preferred_element_type=jnp.float32
    )
    result = result.reshape(width, basis_modes.shape[1], basis_modes.shape[2])
    return (result, factor)


def solution(mesh):
    in_specs = (P(None, ("srv", "grp"), None), P(), P(None, "srv", "grp"))
    out_specs = (P(None, ("srv", "grp"), None), P())
    return jax.shard_map(
        per_device, mesh=mesh, in_specs=in_specs, out_specs=out_specs, check_vma=False
    )
```

```python
import functools
import jax
import jax.numpy as jnp
from jax import lax
from jax.experimental import pallas as pl
from jax.experimental.pallas import tpu as pltpu
from jax.sharding import PartitionSpec as P

AXES = ("srv", "grp")
LANES = 128
TILE = 8
F32, BF16 = jnp.float32, jnp.bfloat16
VMEM = pl.BlockSpec(memory_space=pltpu.VMEM)
ANY = pl.BlockSpec(memory_space=pl.ANY)
PARAMS = pltpu.CompilerParams(vmem_limit_bytes=16 * 2**20)


def total(value):
    servers, cores = lax.axis_size("srv"), lax.axis_size("grp")
    if servers & (servers - 1) or cores != 2:
        return lax.psum(value, AXES)
    count = servers * cores
    masks = [1] + [2 * bit + 1 for bit in (1 << p for p in range(servers.bit_length() - 1))]
    for mask in masks:
        value = value + lax.ppermute(value, AXES, [(i, i ^ mask) for i in range(count)])
    return value


def split(x):
    high = x.astype(BF16)
    return high, (x - high.astype(F32)).astype(BF16)


def rows_times_rows(a, b):
    return lax.dot_general(a, b, (((1,), (1,)), ((), ())), preferred_element_type=F32)


def modes_kernel(modes, panel, gram, buf, sems):
    count, slabs, _ = modes.shape
    chunks = sems.shape[0]
    step = slabs // chunks
    copies = []
    for c in range(chunks):
        part = (slice(None), pl.ds(c * step, step))
        copies.append(pltpu.make_async_copy(modes.at[part], buf.at[part], sems.at[c]))
        copies[-1].start()
    acc = None
    for c in range(chunks):
        copies[c].wait()
        for i in range(c * step, (c + 1) * step):
            high, low = split(buf[:, i, :])
            panel[:count, i * LANES:(i + 1) * LANES] = high
            panel[count:, i * LANES:(i + 1) * LANES] = low
        cols = slice(c * step * LANES, (c + 1) * step * LANES)
        term = rows_times_rows(panel[:, cols], panel[:count, cols])
        acc = term if acc is None else acc + term
    cross = acc[count:]
    gram[...] = acc[:count] + cross + cross.T


def snaps_kernel(first, second, modes_panel, modes_gram, panel, packed):
    snaps, half, _ = first.shape
    modes = modes_gram.shape[0]
    for h, part in enumerate((first, second)):
        for i in range(half):
            high, low = split(part[:, i, :])
            at = (h * half + i) * LANES
            panel[:snaps, at:at + LANES] = high
            panel[snaps:, at:at + LANES] = low
    with_modes = rows_times_rows(panel[...], modes_panel[...])
    own = rows_times_rows(panel[...], panel[:snaps])
    low_row = (with_modes[:snaps, :modes] + with_modes[:snaps, modes:]) + with_modes[snaps:, :modes]
    own = own[:snaps] + own[snaps:] + own[snaps:].T
    width = modes + snaps
    mid = width // 2
    a = modes_gram[...]
    left = jnp.concatenate(
        [
            jnp.concatenate([a[mid:], jnp.zeros((modes - mid, snaps), F32)], axis=1),
            jnp.concatenate([low_row, own], axis=1),
        ],
        axis=0,
    )
    packed[...] = jnp.concatenate(
        [left, a[:mid, :mid], jnp.zeros((mid, LANES - width - mid), F32)], axis=1
    )


def spread_row(x, i):
    return jnp.broadcast_to(x[i:i + 1, :], (TILE, LANES))


def spread_column(x, j):
    return jnp.broadcast_to(x[:, j:j + 1], (x.shape[0], LANES))


def factor_tiles(tiles):
    lane = lax.broadcasted_iota(jnp.int32, (TILE, LANES), 1)
    sub = lax.broadcasted_iota(jnp.int32, (TILE, LANES), 0)
    tiles = list(tiles)
    upper, inverse = [], []
    for t in range(len(tiles)):
        at = t * TILE
        columns = [[spread_column(x, at + j) for j in range(TILE)] for x in tiles[t:]]
        a = {(i, j): spread_row(columns[0][j], i) for j in range(TILE) for i in range(j, TILE)}
        l, m, root = {}, {}, []
        for j in range(TILE):
            r = lax.rsqrt(a[j, j])
            root.append(r)
            for i in range(j + 1, TILE):
                l[i, j] = a[i, j] * r
            for k in range(j + 1, TILE):
                for i in range(k, TILE):
                    a[i, k] = a[i, k] - l[i, j] * l[k, j]
            m[j, j] = r
            for k in range(j):
                dot = l[j, k] * m[k, k]
                for q in range(k + 1, j):
                    dot = dot + l[j, q] * m[q, k]
                m[j, k] = -(dot * r)
        def column_of(k):
            out = jnp.zeros((TILE, LANES), F32)
            for i in range(k, TILE):
                out = jnp.where(sub == i, m[i, k], out)
            return out
        def row_of(i):
            out = jnp.zeros((TILE, LANES), F32)
            for k in range(i + 1):
                out = jnp.where(sub == k, m[i, k], out)
            return out
        m_columns = [column_of(k) for k in range(TILE)]
        row = sum(m_columns[k] * spread_row(tiles[t], k) for k in range(TILE))
        block = (lane >= at) & (lane < at + TILE)
        placed = jnp.zeros((TILE, LANES), F32)
        for k in range(TILE):
            placed = jnp.where(lane == at + k, m_columns[k], placed)
        upper.append(row)
        inv_row = jnp.where(block, placed, jnp.where(lane < at, row, 0.0))
        inverse.append(inv_row)
        if t + 1 == len(tiles):
            break
        mixed = jnp.where(block, placed, row)
        solved = sum(row_of(i) * spread_row(mixed, i) for i in range(TILE))
        rows = [spread_row(solved, j) for j in range(TILE)]
        for s in range(t + 1, len(tiles)):
            x = jnp.where(block, 0.0, tiles[s])
            c = columns[s - t]
            x = x - sum(c[j] * rows[j] for j in range(TILE))
            tiles[s] = x
    return upper, inverse


def apply_kernel(cells, packed, scale, modes_panel, snaps_panel, out, factor, left, buf, sems):
    modes, snaps = modes_panel.shape[0] // 2, snaps_panel.shape[0] // 2
    width = modes + snaps
    mid = width // 2
    both = packed[...] * (1.0 / cells)
    lane = lax.broadcasted_iota(jnp.int32, (mid, LANES), 1)
    top = jnp.where(lane < mid, pltpu.roll(both, LANES - width, 1), 0.0)
    low = jnp.where(lane < width, both, 0.0)
    lower = jnp.concatenate([top, low, jnp.zeros((LANES - width, LANES), F32)], axis=0)
    r = lax.broadcasted_iota(jnp.int32, (LANES, LANES), 0)
    c = lax.broadcasted_iota(jnp.int32, (LANES, LANES), 1)
    full = jnp.where(r >= c, lower, lower.T)
    upper, inverse = factor_tiles([full[i:i + TILE] for i in range(0, width, TILE)])
    for i, x in enumerate(inverse):
        left[i * TILE:(i + 1) * TILE, :] = x
    whole = jnp.concatenate(upper + [jnp.zeros((LANES - width, LANES), F32)], axis=0).T
    whole = jnp.where(r >= c, whole, 0.0)[:width, :width]
    factor[...] = whole * scale[...]
    w_high, w_low = split(left[:, :width])
    wm = jnp.concatenate([w_high[:, :modes], w_low[:, :modes]], axis=0)
    ws = jnp.concatenate([w_high[:, modes:], w_low[:, modes:]], axis=0)
    both_w = jnp.concatenate([wm, wm, ws, ws], axis=1)
    chunks = sems.shape[0]
    slabs = buf.shape[1]
    step = slabs // chunks
    copies = []
    for k in range(chunks):
        cols = slice(k * step * LANES, (k + 1) * step * LANES)
        right = jnp.concatenate([modes_panel[:, cols], snaps_panel[:, cols]], axis=0)
        res = jnp.dot(both_w, right, preferred_element_type=F32)
        res = res[:width] + res[width:]
        for i in range(step):
            buf[:, k * step + i, :] = res[:, i * LANES:(i + 1) * LANES]
        part = (slice(None), pl.ds(k * step, step))
        copies.append(pltpu.make_async_copy(buf.at[part], out.at[part], sems.at[k]))
        copies[-1].start()
    for copy in copies:
        copy.wait()


def per_device(basis_modes, weights, snapshots):
    modes, rows, cols = basis_modes.shape
    snaps = snapshots.shape[0]
    width = modes + snaps
    tiles = cols // LANES
    slabs = rows * tiles
    cores = lax.axis_size("grp")
    cells = rows * cols * lax.axis_size("srv") * cores
    core = lax.axis_index("grp")
    fields = basis_modes.reshape(modes, rows, tiles, LANES).transpose(0, 2, 1, 3)
    fields = fields.reshape(modes, slabs, LANES)
    own = snapshots.reshape(snaps, cores, rows, tiles // cores, LANES).transpose(0, 3, 1, 2, 4)
    keep = jnp.where(core == 0, own[:, :, 0], own[:, :, 1]).reshape(snaps, slabs // cores, LANES)
    send = jnp.where(core == 0, own[:, :, 1], own[:, :, 0]).reshape(snaps, slabs // cores, LANES)
    got = lax.ppermute(send, "grp", [(0, 1), (1, 0)])
    first = jnp.where(core == 0, keep, got)
    second = jnp.where(core == 0, got, keep)

    chunk = 6
    modes_panel, modes_gram = pl.pallas_call(
        modes_kernel,
        out_shape=(
            jax.ShapeDtypeStruct((2 * modes, slabs * LANES), BF16),
            jax.ShapeDtypeStruct((modes, modes), F32),
        ),
        in_specs=[ANY],
        out_specs=(VMEM, VMEM),
        scratch_shapes=[pltpu.VMEM((modes, slabs, LANES), F32), pltpu.SemaphoreType.DMA((chunk,))],
        cost_estimate=pl.CostEstimate(flops=10**8, bytes_accessed=fields.size * 4, transcendentals=0),
        compiler_params=PARAMS,
        name="modes_gram",
    )(fields)
    snaps_panel, packed = pl.pallas_call(
        snaps_kernel,
        out_shape=(
            jax.ShapeDtypeStruct((2 * snaps, slabs * LANES), BF16),
            jax.ShapeDtypeStruct((width // 2, LANES), F32),
        ),
        in_specs=[VMEM] * 4,
        out_specs=(VMEM, VMEM),
        compiler_params=PARAMS,
        name="snaps_gram",
    )(first, second, modes_panel, modes_gram)
    packed = total(packed)
    scale = jnp.concatenate([weights, jnp.ones((snaps,), F32)])
    new_modes, factor = pl.pallas_call(
        functools.partial(apply_kernel, cells),
        out_shape=(
            jax.ShapeDtypeStruct((width, slabs, LANES), F32),
            jax.ShapeDtypeStruct((width, width), F32),
        ),
        in_specs=[VMEM] * 4,
        out_specs=(ANY, VMEM),
        scratch_shapes=[
            pltpu.VMEM((width, LANES), F32),
            pltpu.VMEM((width, slabs, LANES), F32),
            pltpu.SemaphoreType.DMA((chunk,)),
        ],
        compiler_params=PARAMS,
        name="factor_apply",
    )(packed, scale[:, None], modes_panel, snaps_panel)
    new_modes = new_modes.reshape(width, tiles, rows, LANES).transpose(0, 2, 1, 3)
    return new_modes.reshape(width, rows, cols), factor


def solution(mesh):
    in_specs = (P(None, AXES, None), P(), P(None, "srv", "grp"))
    out_specs = (P(None, AXES, None), P())
    return jax.shard_map(
        per_device, mesh=mesh, in_specs=in_specs, out_specs=out_specs, check_vma=False
    )
```

```python
import functools
import jax
import jax.numpy as jnp
from jax import lax
from jax.experimental import pallas as pl
from jax.experimental.pallas import tpu as pltpu
from jax.sharding import PartitionSpec as P

AXES = ("srv", "grp")
LANES = 128
TILE = 8
F32, BF16 = jnp.float32, jnp.bfloat16
VMEM = pl.BlockSpec(memory_space=pltpu.VMEM)
ANY = pl.BlockSpec(memory_space=pl.ANY)
PARAMS = pltpu.CompilerParams(vmem_limit_bytes=16 * 2**20)


def total(value):
    servers, cores = lax.axis_size("srv"), lax.axis_size("grp")
    if servers & (servers - 1) or cores != 2:
        return lax.psum(value, AXES)
    count = servers * cores
    masks = [1] + [2 * bit + 1 for bit in (1 << p for p in range(servers.bit_length() - 1))]
    for mask in masks:
        value = value + lax.ppermute(value, AXES, [(i, i ^ mask) for i in range(count)])
    return value


def split(x):
    high = x.astype(BF16)
    return high, (x - high.astype(F32)).astype(BF16)


def rows_times_rows(a, b):
    return lax.dot_general(a, b, (((1,), (1,)), ((), ())), preferred_element_type=F32)


def modes_kernel(modes, panel, gram):
    count = gram.shape[0]
    slabs = modes.shape[0] // count
    for i in range(slabs):
        high, low = split(modes[pl.ds(i, count, stride=slabs), :])
        panel[:count, i * LANES:(i + 1) * LANES] = high
        panel[count:, i * LANES:(i + 1) * LANES] = low
    acc = rows_times_rows(panel[...], panel[:count])
    cross = acc[count:]
    gram[...] = acc[:count] + cross + cross.T


def snaps_kernel(first, second, modes_panel, modes_gram, panel, packed):
    snaps, modes = panel.shape[0] // 2, modes_gram.shape[0]
    half = first.shape[0] // snaps
    for h, part in enumerate((first, second)):
        for i in range(half):
            high, low = split(part[pl.ds(i, snaps, stride=half), :])
            at = (h * half + i) * LANES
            panel[:snaps, at:at + LANES] = high
            panel[snaps:, at:at + LANES] = low
    with_modes = rows_times_rows(panel[...], modes_panel[...])
    own = rows_times_rows(panel[...], panel[:snaps])
    low_row = (with_modes[:snaps, :modes] + with_modes[:snaps, modes:]) + with_modes[snaps:, :modes]
    own = own[:snaps] + own[snaps:] + own[snaps:].T
    width = modes + snaps
    mid = width // 2
    a = modes_gram[...]
    left = jnp.concatenate(
        [
            jnp.concatenate([a[mid:], jnp.zeros((modes - mid, snaps), F32)], axis=1),
            jnp.concatenate([low_row, own], axis=1),
        ],
        axis=0,
    )
    packed[...] = jnp.concatenate(
        [left, a[:mid, :mid], jnp.zeros((mid, LANES - width - mid), F32)], axis=1
    )


def spread_row(x, i):
    return jnp.broadcast_to(x[i:i + 1, :], (TILE, LANES))


def spread_column(x, j):
    return jnp.broadcast_to(x[:, j:j + 1], (x.shape[0], LANES))


def factor_tiles(tiles):
    lane = lax.broadcasted_iota(jnp.int32, (TILE, LANES), 1)
    sub = lax.broadcasted_iota(jnp.int32, (TILE, LANES), 0)
    tiles = list(tiles)
    upper, inverse = [], []
    for t in range(len(tiles)):
        at = t * TILE
        columns = [[spread_column(x, at + j) for j in range(TILE)] for x in tiles[t:]]
        a = {(i, j): spread_row(columns[0][j], i) for j in range(TILE) for i in range(j, TILE)}
        l, m, root = {}, {}, []
        for j in range(TILE):
            r = lax.rsqrt(a[j, j])
            root.append(r)
            for i in range(j + 1, TILE):
                l[i, j] = a[i, j] * r
            for k in range(j + 1, TILE):
                for i in range(k, TILE):
                    a[i, k] = a[i, k] - l[i, j] * l[k, j]
            m[j, j] = r
            for k in range(j):
                dot = l[j, k] * m[k, k]
                for q in range(k + 1, j):
                    dot = dot + l[j, q] * m[q, k]
                m[j, k] = -(dot * r)
        def column_of(k):
            out = jnp.zeros((TILE, LANES), F32)
            for i in range(k, TILE):
                out = jnp.where(sub == i, m[i, k], out)
            return out
        def row_of(i):
            out = jnp.zeros((TILE, LANES), F32)
            for k in range(i + 1):
                out = jnp.where(sub == k, m[i, k], out)
            return out
        m_columns = [column_of(k) for k in range(TILE)]
        row = sum(m_columns[k] * spread_row(tiles[t], k) for k in range(TILE))
        block = (lane >= at) & (lane < at + TILE)
        placed = jnp.zeros((TILE, LANES), F32)
        for k in range(TILE):
            placed = jnp.where(lane == at + k, m_columns[k], placed)
        upper.append(row)
        inv_row = jnp.where(block, placed, jnp.where(lane < at, row, 0.0))
        inverse.append(inv_row)
        if t + 1 == len(tiles):
            break
        mixed = jnp.where(block, placed, row)
        solved = sum(row_of(i) * spread_row(mixed, i) for i in range(TILE))
        rows = [spread_row(solved, j) for j in range(TILE)]
        for s in range(t + 1, len(tiles)):
            x = jnp.where(block, 0.0, tiles[s])
            c = columns[s - t]
            x = x - sum(c[j] * rows[j] for j in range(TILE))
            tiles[s] = x
    return upper, inverse


def apply_kernel(cells, packed, scale, modes_panel, snaps_panel, out, factor, left, buf, sems):
    modes, snaps = modes_panel.shape[0] // 2, snaps_panel.shape[0] // 2
    width = modes + snaps
    mid = width // 2
    both = packed[...] * (1.0 / cells)
    lane = lax.broadcasted_iota(jnp.int32, (mid, LANES), 1)
    top = jnp.where(lane < mid, pltpu.roll(both, LANES - width, 1), 0.0)
    low = jnp.where(lane < width, both, 0.0)
    lower = jnp.concatenate([top, low, jnp.zeros((LANES - width, LANES), F32)], axis=0)
    r = lax.broadcasted_iota(jnp.int32, (LANES, LANES), 0)
    c = lax.broadcasted_iota(jnp.int32, (LANES, LANES), 1)
    full = jnp.where(r >= c, lower, lower.T)
    upper, inverse = factor_tiles([full[i:i + TILE] for i in range(0, width, TILE)])
    for i, x in enumerate(inverse):
        left[i * TILE:(i + 1) * TILE, :] = x
    whole = jnp.concatenate(upper + [jnp.zeros((LANES - width, LANES), F32)], axis=0).T
    whole = jnp.where(r >= c, whole, 0.0)[:width, :width]
    factor[...] = whole * scale[...]
    w_high, w_low = split(left[:, :width])
    wm = jnp.concatenate([w_high[:, :modes], w_low[:, :modes]], axis=0)
    ws = jnp.concatenate([w_high[:, modes:], w_low[:, modes:]], axis=0)
    both_w = jnp.concatenate([wm, wm, ws, ws], axis=1)
    chunks = sems.shape[0]
    slabs = buf.shape[0] // width
    step = slabs // chunks
    copies = []
    for k in range(chunks):
        cols = slice(k * step * LANES, (k + 1) * step * LANES)
        right = jnp.concatenate([modes_panel[:, cols], snaps_panel[:, cols]], axis=0)
        res = jnp.dot(both_w, right, preferred_element_type=F32)
        res = res[:width] + res[width:]
        for i in range(step):
            buf[pl.ds(k * step + i, width, stride=slabs), :] = res[:, i * LANES:(i + 1) * LANES]
    copy = pltpu.make_async_copy(buf, out, sems.at[0])
    copy.start()
    copy.wait()


def per_device(basis_modes, weights, snapshots):
    modes, rows, cols = basis_modes.shape
    snaps = snapshots.shape[0]
    width = modes + snaps
    tiles = cols // LANES
    slabs = rows * tiles
    cores = lax.axis_size("grp")
    cells = rows * cols * lax.axis_size("srv") * cores
    core = lax.axis_index("grp")
    fields = basis_modes.reshape(modes, rows, tiles, LANES).transpose(0, 2, 1, 3)
    fields = fields.reshape(modes * slabs, LANES)
    own = snapshots.reshape(snaps, cores, rows, tiles // cores, LANES).transpose(0, 3, 1, 2, 4)
    keep = jnp.where(core == 0, own[:, :, 0], own[:, :, 1]).reshape(snaps * slabs // cores, LANES)
    send = jnp.where(core == 0, own[:, :, 1], own[:, :, 0]).reshape(snaps * slabs // cores, LANES)
    got = lax.ppermute(send, "grp", [(0, 1), (1, 0)])
    first = jnp.where(core == 0, keep, got)
    second = jnp.where(core == 0, got, keep)

    chunk = 6
    modes_panel, modes_gram = pl.pallas_call(
        modes_kernel,
        out_shape=(
            jax.ShapeDtypeStruct((2 * modes, slabs * LANES), BF16),
            jax.ShapeDtypeStruct((modes, modes), F32),
        ),
        in_specs=[VMEM],
        out_specs=(VMEM, VMEM),
        cost_estimate=pl.CostEstimate(flops=10**8, bytes_accessed=fields.size * 4, transcendentals=0),
        compiler_params=PARAMS,
        name="modes_gram",
    )(fields)
    snaps_panel, packed = pl.pallas_call(
        snaps_kernel,
        out_shape=(
            jax.ShapeDtypeStruct((2 * snaps, slabs * LANES), BF16),
            jax.ShapeDtypeStruct((width // 2, LANES), F32),
        ),
        in_specs=[VMEM] * 4,
        out_specs=(VMEM, VMEM),
        compiler_params=PARAMS,
        name="snaps_gram",
    )(first, second, modes_panel, modes_gram)
    packed = total(packed)
    scale = jnp.concatenate([weights, jnp.ones((snaps,), F32)])
    new_modes, factor = pl.pallas_call(
        functools.partial(apply_kernel, cells),
        out_shape=(
            jax.ShapeDtypeStruct((width * slabs, LANES), F32),
            jax.ShapeDtypeStruct((width, width), F32),
        ),
        in_specs=[VMEM] * 4,
        out_specs=(ANY, VMEM),
        scratch_shapes=[
            pltpu.VMEM((width, LANES), F32),
            pltpu.VMEM((width * slabs, LANES), F32),
            pltpu.SemaphoreType.DMA((chunk,)),
        ],
        compiler_params=PARAMS,
        name="factor_apply",
    )(packed, scale[:, None], modes_panel, snaps_panel)
    new_modes = new_modes.reshape(width, tiles, rows, LANES).transpose(0, 2, 1, 3)
    return new_modes.reshape(width, rows, cols), factor


def solution(mesh):
    in_specs = (P(None, AXES, None), P(), P(None, "srv", "grp"))
    out_specs = (P(None, AXES, None), P())
    return jax.shard_map(
        per_device, mesh=mesh, in_specs=in_specs, out_specs=out_specs, check_vma=False
    )
```

```python
import functools
import jax
import jax.numpy as jnp
from jax import lax
from jax.experimental.layout import Layout, with_layout_constraint
from jax.experimental import pallas as pl
from jax.experimental.pallas import tpu as pltpu
from jax.sharding import PartitionSpec as P

AXES = ("srv", "grp")
LANES = 128
TILE = 8
F32, BF16 = jnp.float32, jnp.bfloat16
VMEM = pl.BlockSpec(memory_space=pltpu.VMEM)
ANY = pl.BlockSpec(memory_space=pl.ANY)
PARAMS = pltpu.CompilerParams(vmem_limit_bytes=16 * 2**20)


def total(value):
    servers, cores = lax.axis_size("srv"), lax.axis_size("grp")
    if servers & (servers - 1) or cores != 2:
        return lax.psum(value, AXES)
    count = servers * cores
    masks = [1] + [2 * bit + 1 for bit in (1 << p for p in range(servers.bit_length() - 1))]
    for mask in masks:
        value = value + lax.ppermute(value, AXES, [(i, i ^ mask) for i in range(count)])
    return value


def split(x):
    high = x.astype(BF16)
    return high, (x - high.astype(F32)).astype(BF16)


def rows_times_rows(a, b):
    return lax.dot_general(a, b, (((1,), (1,)), ((), ())), preferred_element_type=F32)


def modes_kernel(modes, panel, gram):
    count = gram.shape[0]
    slabs = modes.shape[0] // count
    for i in range(slabs):
        high, low = split(modes[pl.ds(i, count, stride=slabs), :])
        panel[:count, i * LANES:(i + 1) * LANES] = high
        panel[count:, i * LANES:(i + 1) * LANES] = low
    acc = rows_times_rows(panel[...], panel[:count])
    cross = acc[count:]
    gram[...] = acc[:count] + cross + cross.T


def pick_kernel(rows, snaps, keep, send):
    core = lax.axis_index("grp")
    count = keep.shape[0] // rows
    stride = snaps.shape[0] // count
    for r in range(rows):
        at = slice(r * count, (r + 1) * count)
        keep[at] = snaps[pl.ds(core * rows + r, count, stride=stride), :]
        send[at] = snaps[pl.ds((1 - core) * rows + r, count, stride=stride), :]


def snaps_kernel(rows, first, second, modes_panel, modes_gram, panel, packed):
    snaps, modes = panel.shape[0] // 2, modes_gram.shape[0]
    tiles = first.shape[0] // (snaps * rows)
    for h, part in enumerate((first, second)):
        for i in range(tiles * rows):
            start = (i % rows) * snaps * tiles + i // rows
            high, low = split(part[pl.ds(start, snaps, stride=tiles), :])
            at = (h * tiles * rows + i) * LANES
            panel[:snaps, at:at + LANES] = high
            panel[snaps:, at:at + LANES] = low
    with_modes = rows_times_rows(modes_panel[...], panel[...])
    own = rows_times_rows(panel[...], panel[:snaps])
    top = with_modes[:modes]
    low_row = (top[:, :snaps] + top[:, snaps:] + with_modes[modes:, :snaps]).T
    own = own[:snaps] + own[snaps:] + own[snaps:].T
    width = modes + snaps
    mid = width // 2
    a = modes_gram[...]
    left = jnp.concatenate(
        [
            jnp.concatenate([a[mid:], jnp.zeros((modes - mid, snaps), F32)], axis=1),
            jnp.concatenate([low_row, own], axis=1),
        ],
        axis=0,
    )
    packed[...] = jnp.concatenate(
        [left, a[:mid, :mid], jnp.zeros((mid, LANES - width - mid), F32)], axis=1
    )


def spread_row(x, i):
    return jnp.broadcast_to(x[i:i + 1, :], (TILE, LANES))


def spread_column(x, j):
    return jnp.broadcast_to(x[:, j:j + 1], (x.shape[0], LANES))


def factor_tiles(tiles):
    lane = lax.broadcasted_iota(jnp.int32, (TILE, LANES), 1)
    sub = lax.broadcasted_iota(jnp.int32, (TILE, LANES), 0)
    tiles = list(tiles)
    upper, inverse = [], []
    for t in range(len(tiles)):
        at = t * TILE
        columns = [[spread_column(x, at + j) for j in range(TILE)] for x in tiles[t:]]
        a = {(i, j): spread_row(columns[0][j], i) for j in range(TILE) for i in range(j, TILE)}
        l, m, root = {}, {}, []
        for j in range(TILE):
            r = lax.rsqrt(a[j, j])
            root.append(r)
            for i in range(j + 1, TILE):
                l[i, j] = a[i, j] * r
            for k in range(j + 1, TILE):
                for i in range(k, TILE):
                    a[i, k] = a[i, k] - l[i, j] * l[k, j]
            m[j, j] = r
            for k in range(j):
                dot = l[j, k] * m[k, k]
                for q in range(k + 1, j):
                    dot = dot + l[j, q] * m[q, k]
                m[j, k] = -(dot * r)
        def column_of(k):
            out = jnp.zeros((TILE, LANES), F32)
            for i in range(k, TILE):
                out = jnp.where(sub == i, m[i, k], out)
            return out
        def row_of(i):
            out = jnp.zeros((TILE, LANES), F32)
            for k in range(i + 1):
                out = jnp.where(sub == k, m[i, k], out)
            return out
        m_columns = [column_of(k) for k in range(TILE)]
        row = sum(m_columns[k] * spread_row(tiles[t], k) for k in range(TILE))
        block = (lane >= at) & (lane < at + TILE)
        placed = jnp.zeros((TILE, LANES), F32)
        for k in range(TILE):
            placed = jnp.where(lane == at + k, m_columns[k], placed)
        upper.append(row)
        inv_row = jnp.where(block, placed, jnp.where(lane < at, row, 0.0))
        inverse.append(inv_row)
        if t + 1 == len(tiles):
            break
        mixed = jnp.where(block, placed, row)
        solved = sum(row_of(i) * spread_row(mixed, i) for i in range(TILE))
        rows = [spread_row(solved, j) for j in range(TILE)]
        for s in range(t + 1, len(tiles)):
            x = jnp.where(block, 0.0, tiles[s])
            c = columns[s - t]
            x = x - sum(c[j] * rows[j] for j in range(TILE))
            tiles[s] = x
    return upper, inverse


def apply_kernel(cells, packed, scale, modes_panel, snaps_panel, out, factor, left, buf, sems):
    modes, snaps = modes_panel.shape[0] // 2, snaps_panel.shape[0] // 2
    width = modes + snaps
    mid = width // 2
    both = packed[...] * (1.0 / cells)
    lane = lax.broadcasted_iota(jnp.int32, (mid, LANES), 1)
    top = jnp.where(lane < mid, pltpu.roll(both, LANES - width, 1), 0.0)
    low = jnp.where(lane < width, both, 0.0)
    lower = jnp.concatenate([top, low, jnp.zeros((LANES - width, LANES), F32)], axis=0)
    r = lax.broadcasted_iota(jnp.int32, (LANES, LANES), 0)
    c = lax.broadcasted_iota(jnp.int32, (LANES, LANES), 1)
    full = jnp.where(r >= c, lower, lower.T)
    upper, inverse = factor_tiles([full[i:i + TILE] for i in range(0, width, TILE)])
    for i, x in enumerate(inverse):
        left[i * TILE:(i + 1) * TILE, :] = x
    whole = jnp.concatenate(upper + [jnp.zeros((LANES - width, LANES), F32)], axis=0).T
    whole = jnp.where(r >= c, whole, 0.0)[:width, :width]
    factor[...] = whole * scale[...]
    w_high, w_low = split(left[:, :width])
    wm = jnp.concatenate([w_high[:, :modes], w_low[:, :modes]], axis=0)
    ws = jnp.concatenate([w_high[:, modes:], w_low[:, modes:]], axis=0)
    both_w = jnp.concatenate([wm, wm, ws, ws], axis=1)
    chunks = sems.shape[0]
    slabs = buf.shape[1]
    flat = buf.reshape(width * slabs, LANES)
    step = slabs // chunks
    copies = []
    for k in range(chunks):
        cols = slice(k * step * LANES, (k + 1) * step * LANES)
        right = jnp.concatenate([modes_panel[:, cols], snaps_panel[:, cols]], axis=0)
        res = jnp.dot(both_w, right, preferred_element_type=F32)
        res = res[:width] + res[width:]
        for i in range(step):
            flat[pl.ds(k * step + i, width, stride=slabs), :] = res[:, i * LANES:(i + 1) * LANES]
        part = (slice(None), pl.ds(k * step, step))
        copies.append(pltpu.make_async_copy(buf.at[part], out.at[part], sems.at[k]))
        copies[-1].start()
    for copy in copies:
        copy.wait()


def per_device(basis_modes, weights, snapshots):
    modes, rows, cols = basis_modes.shape
    snaps = snapshots.shape[0]
    width = modes + snaps
    tiles = cols // LANES
    slabs = rows * tiles
    cores = lax.axis_size("grp")
    cells = rows * cols * lax.axis_size("srv") * cores
    core = lax.axis_index("grp")
    fields = basis_modes.reshape(modes, rows, tiles, LANES).transpose(0, 2, 1, 3)
    fields = fields.reshape(modes * slabs, LANES)
    own = snapshots.reshape(snaps, cores * rows, tiles // cores, LANES)
    own = with_layout_constraint(own, Layout((0, 2, 1, 3))).transpose(0, 2, 1, 3)
    own = own.reshape(snaps * tiles * rows, LANES)
    part = jax.ShapeDtypeStruct((own.shape[0] // cores, LANES), F32)
    keep, send = pl.pallas_call(
        functools.partial(pick_kernel, rows),
        out_shape=(part, part),
        in_specs=[VMEM],
        out_specs=(VMEM, VMEM),
        compiler_params=PARAMS,
        name="pick_rows",
    )(own)
    got = lax.ppermute(send, "grp", [(0, 1), (1, 0)])
    first = jnp.where(core == 0, keep, got)
    second = jnp.where(core == 0, got, keep)

    chunk = 6
    modes_panel, modes_gram = pl.pallas_call(
        modes_kernel,
        out_shape=(
            jax.ShapeDtypeStruct((2 * modes, slabs * LANES), BF16),
            jax.ShapeDtypeStruct((modes, modes), F32),
        ),
        in_specs=[VMEM],
        out_specs=(VMEM, VMEM),
        cost_estimate=pl.CostEstimate(flops=10**8, bytes_accessed=fields.size * 4, transcendentals=0),
        compiler_params=PARAMS,
        name="modes_gram",
    )(fields)
    snaps_panel, packed = pl.pallas_call(
        functools.partial(snaps_kernel, rows),
        out_shape=(
            jax.ShapeDtypeStruct((2 * snaps, slabs * LANES), BF16),
            jax.ShapeDtypeStruct((width // 2, LANES), F32),
        ),
        in_specs=[VMEM] * 4,
        out_specs=(VMEM, VMEM),
        compiler_params=PARAMS,
        name="snaps_gram",
    )(first, second, modes_panel, modes_gram)
    packed = total(packed)
    scale = jnp.concatenate([weights, jnp.ones((snaps,), F32)])
    new_modes, factor = pl.pallas_call(
        functools.partial(apply_kernel, cells),
        out_shape=(
            jax.ShapeDtypeStruct((width, slabs, LANES), F32),
            jax.ShapeDtypeStruct((width, width), F32),
        ),
        in_specs=[VMEM] * 4,
        out_specs=(ANY, VMEM),
        scratch_shapes=[
            pltpu.VMEM((width, LANES), F32),
            pltpu.VMEM((width, slabs, LANES), F32),
            pltpu.SemaphoreType.DMA((chunk,)),
        ],
        compiler_params=PARAMS,
        name="factor_apply",
    )(packed, scale[:, None], modes_panel, snaps_panel)
    new_modes = new_modes.reshape(width, tiles, rows, LANES).transpose(0, 2, 1, 3)
    return new_modes.reshape(width, rows, cols), factor


def solution(mesh):
    in_specs = (P(None, AXES, None), P(), P(None, "srv", "grp"))
    out_specs = (P(None, AXES, None), P())
    return jax.shard_map(
        per_device, mesh=mesh, in_specs=in_specs, out_specs=out_specs, check_vma=False
    )
```

```python
import functools
import jax
import jax.numpy as jnp
from jax import lax
from jax.experimental.layout import Layout, with_layout_constraint
from jax.experimental import pallas as pl
from jax.experimental.pallas import tpu as pltpu
from jax.sharding import PartitionSpec as P

AXES = ("srv", "grp")
LANES = 128
TILE = 8
F32, BF16 = jnp.float32, jnp.bfloat16
VMEM = pl.BlockSpec(memory_space=pltpu.VMEM)
ANY = pl.BlockSpec(memory_space=pl.ANY)
HBM = pl.BlockSpec(memory_space=pltpu.HBM)
PARAMS = pltpu.CompilerParams(vmem_limit_bytes=16 * 2**20)


def total(value):
    servers, cores = lax.axis_size("srv"), lax.axis_size("grp")
    if servers & (servers - 1) or cores != 2:
        return lax.psum(value, AXES)
    count = servers * cores
    masks = [1] + [2 * bit + 1 for bit in (1 << p for p in range(servers.bit_length() - 1))]
    for mask in masks:
        value = value + lax.ppermute(value, AXES, [(i, i ^ mask) for i in range(count)])
    return value


def split(x):
    high = x.astype(BF16)
    return high, (x - high.astype(F32)).astype(BF16)


def rows_times_rows(a, b):
    return lax.dot_general(a, b, (((1,), (1,)), ((), ())), preferred_element_type=F32)


def modes_kernel(modes, panel, gram):
    count = gram.shape[0]
    slabs = modes.shape[0] // count
    for i in range(slabs):
        high, low = split(modes[pl.ds(i, count, stride=slabs), :])
        panel[:count, i * LANES:(i + 1) * LANES] = high
        panel[count:, i * LANES:(i + 1) * LANES] = low
    acc = rows_times_rows(panel[...], panel[:count])
    cross = acc[count:]
    gram[...] = acc[:count] + cross + cross.T


def pick_kernel(rows, source, keep, send, snaps, sem):
    copy = pltpu.make_async_copy(source, snaps, sem)
    copy.start()
    copy.wait()
    core = lax.axis_index("grp")
    count = keep.shape[0] // rows
    stride = snaps.shape[0] // count
    for r in range(rows):
        at = slice(r * count, (r + 1) * count)
        keep[at] = snaps[pl.ds(core * rows + r, count, stride=stride), :]
        send[at] = snaps[pl.ds((1 - core) * rows + r, count, stride=stride), :]


def snaps_kernel(rows, keep, got, modes_panel, modes_gram, panel, packed):
    snaps, modes = panel.shape[0] // 2, modes_gram.shape[0]
    tiles = keep.shape[0] // (snaps * rows)
    kept = [lax.axis_index("grp") == h for h in (0, 1)]
    for h in (0, 1):
        for i in range(tiles * rows):
            place = pl.ds((i % rows) * snaps * tiles + i // rows, snaps, stride=tiles)
            high, low = split(jnp.where(kept[h], keep[place, :], got[place, :]))
            at = (h * tiles * rows + i) * LANES
            panel[:snaps, at:at + LANES] = high
            panel[snaps:, at:at + LANES] = low
    with_modes = rows_times_rows(modes_panel[...], panel[...])
    own = rows_times_rows(panel[...], panel[:snaps])
    top = with_modes[:modes]
    low_row = (top[:, :snaps] + top[:, snaps:] + with_modes[modes:, :snaps]).T
    own = own[:snaps] + own[snaps:] + own[snaps:].T
    width = modes + snaps
    mid = width // 2
    a = modes_gram[...]
    left = jnp.concatenate(
        [
            jnp.concatenate([a[mid:], jnp.zeros((modes - mid, snaps), F32)], axis=1),
            jnp.concatenate([low_row, own], axis=1),
        ],
        axis=0,
    )
    packed[...] = jnp.concatenate(
        [left, a[:mid, :mid], jnp.zeros((mid, LANES - width - mid), F32)], axis=1
    )


def spread_row(x, i):
    return jnp.broadcast_to(x[i:i + 1, :], (TILE, LANES))


def spread_column(x, j):
    return jnp.broadcast_to(x[:, j:j + 1], (x.shape[0], LANES))


def factor_tiles(tiles):
    lane = lax.broadcasted_iota(jnp.int32, (TILE, LANES), 1)
    sub = lax.broadcasted_iota(jnp.int32, (TILE, LANES), 0)
    tiles = list(tiles)
    upper, inverse = [], []
    for t in range(len(tiles)):
        at = t * TILE
        columns = [[spread_column(x, at + j) for j in range(TILE)] for x in tiles[t:]]
        a = {(i, j): spread_row(columns[0][j], i) for j in range(TILE) for i in range(j, TILE)}
        l, m, root = {}, {}, []
        for j in range(TILE):
            r = lax.rsqrt(a[j, j])
            root.append(r)
            for i in range(j + 1, TILE):
                l[i, j] = a[i, j] * r
            for k in range(j + 1, TILE):
                for i in range(k, TILE):
                    a[i, k] = a[i, k] - l[i, j] * l[k, j]
            m[j, j] = r
            for k in range(j):
                dot = l[j, k] * m[k, k]
                for q in range(k + 1, j):
                    dot = dot + l[j, q] * m[q, k]
                m[j, k] = -(dot * r)
        def column_of(k):
            out = jnp.zeros((TILE, LANES), F32)
            for i in range(k, TILE):
                out = jnp.where(sub == i, m[i, k], out)
            return out
        def row_of(i):
            out = jnp.zeros((TILE, LANES), F32)
            for k in range(i + 1):
                out = jnp.where(sub == k, m[i, k], out)
            return out
        m_columns = [column_of(k) for k in range(TILE)]
        row = sum(m_columns[k] * spread_row(tiles[t], k) for k in range(TILE))
        block = (lane >= at) & (lane < at + TILE)
        placed = jnp.zeros((TILE, LANES), F32)
        for k in range(TILE):
            placed = jnp.where(lane == at + k, m_columns[k], placed)
        upper.append(row)
        inv_row = jnp.where(block, placed, jnp.where(lane < at, row, 0.0))
        inverse.append(inv_row)
        if t + 1 == len(tiles):
            break
        mixed = jnp.where(block, placed, row)
        solved = sum(row_of(i) * spread_row(mixed, i) for i in range(TILE))
        rows = [spread_row(solved, j) for j in range(TILE)]
        for s in range(t + 1, len(tiles)):
            x = jnp.where(block, 0.0, tiles[s])
            c = columns[s - t]
            x = x - sum(c[j] * rows[j] for j in range(TILE))
            tiles[s] = x
    return upper, inverse


def apply_kernel(cells, packed, scale, modes_panel, snaps_panel, out, factor, left, buf, sems):
    modes, snaps = modes_panel.shape[0] // 2, snaps_panel.shape[0] // 2
    width = modes + snaps
    mid = width // 2
    both = packed[...] * (1.0 / cells)
    lane = lax.broadcasted_iota(jnp.int32, (mid, LANES), 1)
    top = jnp.where(lane < mid, pltpu.roll(both, LANES - width, 1), 0.0)
    low = jnp.where(lane < width, both, 0.0)
    lower = jnp.concatenate([top, low, jnp.zeros((LANES - width, LANES), F32)], axis=0)
    r = lax.broadcasted_iota(jnp.int32, (LANES, LANES), 0)
    c = lax.broadcasted_iota(jnp.int32, (LANES, LANES), 1)
    full = jnp.where(r >= c, lower, lower.T)
    upper, inverse = factor_tiles([full[i:i + TILE] for i in range(0, width, TILE)])
    for i, x in enumerate(inverse):
        left[i * TILE:(i + 1) * TILE, :] = x
    whole = jnp.concatenate(upper + [jnp.zeros((LANES - width, LANES), F32)], axis=0).T
    whole = jnp.where(r >= c, whole, 0.0)[:width, :width]
    factor[...] = whole * scale[...]
    w_high, w_low = split(left[:, :width])
    wm = jnp.concatenate([w_high[:, :modes], w_low[:, :modes]], axis=0)
    ws = jnp.concatenate([w_high[:, modes:], w_low[:, modes:]], axis=0)
    both_w = jnp.concatenate([wm, wm, ws, ws], axis=1)
    chunks = sems.shape[0]
    slabs = buf.shape[1]
    flat = buf.reshape(width * slabs, LANES)
    step = slabs // chunks
    copies = []
    for k in range(chunks):
        cols = slice(k * step * LANES, (k + 1) * step * LANES)
        right = jnp.concatenate([modes_panel[:, cols], snaps_panel[:, cols]], axis=0)
        res = jnp.dot(both_w, right, preferred_element_type=F32)
        res = res[:width] + res[width:]
        for i in range(step):
            flat[pl.ds(k * step + i, width, stride=slabs), :] = res[:, i * LANES:(i + 1) * LANES]
        part = (slice(None), pl.ds(k * step, step))
        copies.append(pltpu.make_async_copy(buf.at[part], out.at[part], sems.at[k]))
        copies[-1].start()
    for copy in copies:
        copy.wait()


def per_device(basis_modes, weights, snapshots):
    modes, rows, cols = basis_modes.shape
    snaps = snapshots.shape[0]
    width = modes + snaps
    tiles = cols // LANES
    slabs = rows * tiles
    cores = lax.axis_size("grp")
    cells = rows * cols * lax.axis_size("srv") * cores
    fields = basis_modes.reshape(modes, rows, tiles, LANES).transpose(0, 2, 1, 3)
    fields = fields.reshape(modes * slabs, LANES)
    own = snapshots.reshape(snaps, cores * rows, tiles // cores, LANES)
    own = with_layout_constraint(own, Layout((0, 2, 1, 3))).transpose(0, 2, 1, 3)
    own = own.reshape(snaps * tiles * rows, LANES)
    own = pltpu.with_memory_space_constraint(own, pltpu.HBM)
    part = jax.ShapeDtypeStruct((own.shape[0] // cores, LANES), F32)
    keep, send = pl.pallas_call(
        functools.partial(pick_kernel, rows),
        out_shape=(part, part),
        in_specs=[HBM],
        out_specs=(VMEM, VMEM),
        scratch_shapes=[pltpu.VMEM(own.shape, F32), pltpu.SemaphoreType.DMA],
        compiler_params=PARAMS,
        cost_estimate=pl.CostEstimate(flops=10**9, bytes_accessed=own.size * 8, transcendentals=0),
        name="pick_rows",
    )(own)
    got = lax.ppermute(send, "grp", [(0, 1), (1, 0)])

    chunk = 6
    modes_panel, modes_gram = pl.pallas_call(
        modes_kernel,
        out_shape=(
            jax.ShapeDtypeStruct((2 * modes, slabs * LANES), BF16),
            jax.ShapeDtypeStruct((modes, modes), F32),
        ),
        in_specs=[VMEM],
        out_specs=(VMEM, VMEM),
        cost_estimate=pl.CostEstimate(flops=10**8, bytes_accessed=fields.size * 4, transcendentals=0),
        compiler_params=PARAMS,
        name="modes_gram",
    )(fields)
    snaps_panel, packed = pl.pallas_call(
        functools.partial(snaps_kernel, rows),
        out_shape=(
            jax.ShapeDtypeStruct((2 * snaps, slabs * LANES), BF16),
            jax.ShapeDtypeStruct((width // 2, LANES), F32),
        ),
        in_specs=[VMEM] * 4,
        out_specs=(VMEM, VMEM),
        compiler_params=PARAMS,
        cost_estimate=pl.CostEstimate(flops=10**8, bytes_accessed=10**6, transcendentals=0),
        name="snaps_gram",
    )(keep, got, modes_panel, modes_gram)
    packed = total(packed)
    scale = jnp.concatenate([weights, jnp.ones((snaps,), F32)])
    new_modes, factor = pl.pallas_call(
        functools.partial(apply_kernel, cells),
        out_shape=(
            jax.ShapeDtypeStruct((width, slabs, LANES), F32),
            jax.ShapeDtypeStruct((width, width), F32),
        ),
        in_specs=[VMEM] * 4,
        out_specs=(ANY, VMEM),
        scratch_shapes=[
            pltpu.VMEM((width, LANES), F32),
            pltpu.VMEM((width, slabs, LANES), F32),
            pltpu.SemaphoreType.DMA((chunk,)),
        ],
        compiler_params=PARAMS,
        name="factor_apply",
    )(packed, scale[:, None], modes_panel, snaps_panel)
    new_modes = new_modes.reshape(width, tiles, rows, LANES).transpose(0, 2, 1, 3)
    return new_modes.reshape(width, rows, cols), factor


def solution(mesh):
    in_specs = (P(None, AXES, None), P(), P(None, "srv", "grp"))
    out_specs = (P(None, AXES, None), P())
    return jax.shard_map(
        per_device, mesh=mesh, in_specs=in_specs, out_specs=out_specs, check_vma=False
    )
```

```python
import functools
import jax
import jax.numpy as jnp
from jax import lax
from jax.experimental.layout import Layout, with_layout_constraint
from jax.experimental import pallas as pl
from jax.experimental.pallas import tpu as pltpu
from jax.sharding import PartitionSpec as P

AXES = ("srv", "grp")
LANES = 128
TILE = 8
F32, BF16 = jnp.float32, jnp.bfloat16
VMEM = pl.BlockSpec(memory_space=pltpu.VMEM)
ANY = pl.BlockSpec(memory_space=pl.ANY)
HBM = pl.BlockSpec(memory_space=pltpu.HBM)
PARAMS = pltpu.CompilerParams(vmem_limit_bytes=16 * 2**20)


def total(value):
    servers, cores = lax.axis_size("srv"), lax.axis_size("grp")
    if servers & (servers - 1) or cores != 2:
        return lax.psum(value, AXES)
    count = servers * cores
    masks = [1] + [2 * bit + 1 for bit in (1 << p for p in range(servers.bit_length() - 1))]
    for mask in masks:
        value = value + lax.ppermute(value, AXES, [(i, i ^ mask) for i in range(count)])
    return value


def split(x):
    high = x.astype(BF16)
    return high, (x - high.astype(F32)).astype(BF16)


def rows_times_rows(a, b):
    return lax.dot_general(a, b, (((1,), (1,)), ((), ())), preferred_element_type=F32)


def modes_kernel(modes, panel, gram):
    count = gram.shape[0]
    slabs = modes.shape[0] // count
    for i in range(slabs):
        high, low = split(modes[pl.ds(i, count, stride=slabs), :])
        panel[:count, i * LANES:(i + 1) * LANES] = high
        panel[count:, i * LANES:(i + 1) * LANES] = low
    acc = rows_times_rows(panel[...], panel[:count])
    cross = acc[count:]
    gram[...] = acc[:count] + cross + cross.T


def pick_kernel(rows, source, keep, send, snaps, sem):
    copy = pltpu.make_async_copy(source, snaps, sem)
    copy.start()
    copy.wait()
    core = lax.axis_index("grp")
    count = keep.shape[0] // rows
    stride = snaps.shape[0] // count
    for r in range(rows):
        at = slice(r * count, (r + 1) * count)
        keep[at] = snaps[pl.ds(core * rows + r, count, stride=stride), :]
        send[at] = snaps[pl.ds((1 - core) * rows + r, count, stride=stride), :]


def snaps_kernel(rows, keep, got, modes_panel, modes_gram, panel, packed):
    snaps, modes = panel.shape[0] // 2, modes_gram.shape[0]
    tiles = keep.shape[0] // (snaps * rows)
    kept = [lax.axis_index("grp") == h for h in (0, 1)]
    for h in (0, 1):
        for i in range(tiles * rows):
            place = pl.ds((i % rows) * snaps * tiles + i // rows, snaps, stride=tiles)
            high, low = split(jnp.where(kept[h], keep[place, :], got[place, :]))
            at = (h * tiles * rows + i) * LANES
            panel[:snaps, at:at + LANES] = high
            panel[snaps:, at:at + LANES] = low
    with_modes = rows_times_rows(modes_panel[...], panel[...])
    own = rows_times_rows(panel[...], panel[:snaps])
    top = with_modes[:modes]
    low_row = (top[:, :snaps] + top[:, snaps:] + with_modes[modes:, :snaps]).T
    own = own[:snaps] + own[snaps:] + own[snaps:].T
    width = modes + snaps
    mid = width // 2
    a = modes_gram[...]
    left = jnp.concatenate(
        [
            jnp.concatenate([a[mid:], jnp.zeros((modes - mid, snaps), F32)], axis=1),
            jnp.concatenate([low_row, own], axis=1),
        ],
        axis=0,
    )
    packed[...] = jnp.concatenate(
        [left, a[:mid, :mid], jnp.zeros((mid, LANES - width - mid), F32)], axis=1
    )


def spread_row(x, i):
    return jnp.broadcast_to(x[i:i + 1, :], (TILE, LANES))


def spread_column(x, j):
    return jnp.broadcast_to(x[:, j:j + 1], (x.shape[0], LANES))


def total_of(terms):
    terms = list(terms)
    while len(terms) > 1:
        terms = [sum(terms[i:i + 2]) for i in range(0, len(terms), 2)]
    return terms[0]


def everywhere(ref, row):
    return jnp.broadcast_to(ref[row:row + 1, :], (TILE, LANES))


def block_inverse(a):
    a = dict(a)
    l, m = {}, {}
    for p in range(0, TILE, 2):
        q = p + 1
        root = lax.rsqrt(a[p, p])
        det = a[p, p] * a[q, q] - a[q, p] * a[q, p]
        root_det = lax.rsqrt(det)
        over_det = root_det * root_det
        m[p, p] = root
        m[q, q] = root_det * (a[p, p] * root)
        l[q, p] = a[q, p] * root
        both = root_det * root
        w, z = {}, {}
        for i in range(q + 1, TILE):
            w[i] = a[p, p] * a[i, q] - a[q, p] * a[i, p]
            z[i] = a[q, q] * a[i, p] - a[q, p] * a[i, q]
            l[i, p] = a[i, p] * root
            l[i, q] = w[i] * both
        for k in range(q + 1, TILE):
            for i in range(k, TILE):
                a[i, k] = a[i, k] - (a[i, p] * z[k] + a[i, q] * w[k]) * over_det
        for i in (p, q):
            for k in range(i):
                m[i, k] = -m[i, i] * total_of(l[i, j] * m[j, k] for j in range(k, i))
    return m


def factor_tiles(tiles, entries, columns_of, rows_of, solved_of):
    count = len(tiles)
    lane = lax.broadcasted_iota(jnp.int32, (TILE, LANES), 1)
    tiles = list(tiles)
    upper, inverse = [], []
    square = TILE * TILE
    for b in range(2):
        columns_of[b] = jnp.zeros((square, LANES), F32)
        rows_of[b] = jnp.zeros((square, LANES), F32)
    diagonal = [spread_column(tiles[0], j) for j in range(TILE)]
    below = [[spread_column(x, j) for j in range(TILE)] for x in tiles[1:]]
    following = [spread_column(tiles[1], TILE + j) for j in range(TILE)]
    for t in range(count):
        at = t * TILE
        slot = entries.at[t]
        for j in range(TILE):
            slot[j * TILE:(j + 1) * TILE, :] = diagonal[j]
        m = block_inverse(
            {(i, j): everywhere(slot, j * TILE + i) for j in range(TILE) for i in range(j, TILE)}
        )
        if t + 1 < count:
            ahead = solved_of.at[t]
            for i in range(TILE):
                solved = total_of(m[i, j] * below[0][j] for j in range(i + 1))
                ahead[i * TILE:(i + 1) * TILE, :] = solved
            kept = [ahead[i * TILE:(i + 1) * TILE, :] for i in range(TILE)]
            diagonal = [
                following[k]
                - total_of(kept[i] * everywhere(ahead, i * TILE + k) for i in range(TILE))
                for k in range(TILE)
            ]
        by_column, by_row = columns_of.at[t % 2], rows_of.at[t % 2]
        for i in range(TILE):
            for k in range(i + 1):
                by_column[k * TILE + i:k * TILE + i + 1, :] = m[i, k][:1]
                by_row[i * TILE + k:i * TILE + k + 1, :] = m[i, k][:1]
        m_columns = [by_column[k * TILE:(k + 1) * TILE, :] for k in range(TILE)]
        row = total_of(m_columns[k] * spread_row(tiles[t], k) for k in range(TILE))
        block = (lane >= at) & (lane < at + TILE)
        mixed = row
        for k in range(TILE):
            mixed = jnp.where(lane == at + k, m_columns[k], mixed)
        upper.append(row)
        inverse.append(jnp.where(lane < at + TILE, mixed, 0.0))
        if t + 1 == count:
            break
        solved = total_of(
            by_row[i * TILE:(i + 1) * TILE, :] * spread_row(mixed, i) for i in range(TILE)
        )
        rows = [spread_row(solved, j) for j in range(TILE)]
        for s in range(t + 1, count):
            c = below[s - t - 1]
            tiles[s] = jnp.where(block, 0.0, tiles[s]) - total_of(c[j] * rows[j] for j in range(TILE))
        below = [[spread_column(x, at + TILE + j) for j in range(TILE)] for x in tiles[t + 2:]]
        if t + 2 < count:
            following = [spread_column(tiles[t + 2], at + 2 * TILE + j) for j in range(TILE)]
    return upper, inverse


def apply_kernel(cells, packed, scale, modes_panel, snaps_panel, out, factor, left, buf, sems, *spread):
    modes, snaps = modes_panel.shape[0] // 2, snaps_panel.shape[0] // 2
    width = modes + snaps
    mid = width // 2
    both = packed[...] * (1.0 / cells)
    lane = lax.broadcasted_iota(jnp.int32, (mid, LANES), 1)
    top = jnp.where(lane < mid, pltpu.roll(both, LANES - width, 1), 0.0)
    low = jnp.where(lane < width, both, 0.0)
    lower = jnp.concatenate([top, low, jnp.zeros((LANES - width, LANES), F32)], axis=0)
    r = lax.broadcasted_iota(jnp.int32, (LANES, LANES), 0)
    c = lax.broadcasted_iota(jnp.int32, (LANES, LANES), 1)
    full = jnp.where(r >= c, lower, lower.T)
    upper, inverse = factor_tiles([full[i:i + TILE] for i in range(0, width, TILE)], *spread)
    for i, x in enumerate(inverse):
        left[i * TILE:(i + 1) * TILE, :] = x
    whole = jnp.concatenate(upper + [jnp.zeros((LANES - width, LANES), F32)], axis=0).T
    whole = jnp.where(r >= c, whole, 0.0)[:width, :width]
    factor[...] = whole * scale[...]
    w_high, w_low = split(left[:, :width])
    wm = jnp.concatenate([w_high[:, :modes], w_low[:, :modes]], axis=0)
    ws = jnp.concatenate([w_high[:, modes:], w_low[:, modes:]], axis=0)
    both_w = jnp.concatenate([wm, wm, ws, ws], axis=1)
    chunks = sems.shape[0]
    slabs = buf.shape[1]
    flat = buf.reshape(width * slabs, LANES)
    step = slabs // chunks
    copies = []
    for k in range(chunks):
        cols = slice(k * step * LANES, (k + 1) * step * LANES)
        right = jnp.concatenate([modes_panel[:, cols], snaps_panel[:, cols]], axis=0)
        res = jnp.dot(both_w, right, preferred_element_type=F32)
        res = res[:width] + res[width:]
        for i in range(step):
            flat[pl.ds(k * step + i, width, stride=slabs), :] = res[:, i * LANES:(i + 1) * LANES]
        part = (slice(None), pl.ds(k * step, step))
        copies.append(pltpu.make_async_copy(buf.at[part], out.at[part], sems.at[k]))
        copies[-1].start()
    for copy in copies:
        copy.wait()


def per_device(basis_modes, weights, snapshots):
    modes, rows, cols = basis_modes.shape
    snaps = snapshots.shape[0]
    width = modes + snaps
    tiles = cols // LANES
    slabs = rows * tiles
    cores = lax.axis_size("grp")
    cells = rows * cols * lax.axis_size("srv") * cores
    fields = basis_modes.reshape(modes, rows, tiles, LANES).transpose(0, 2, 1, 3)
    fields = fields.reshape(modes * slabs, LANES)
    own = snapshots.reshape(snaps, cores * rows, tiles // cores, LANES)
    own = with_layout_constraint(own, Layout((0, 2, 1, 3))).transpose(0, 2, 1, 3)
    own = own.reshape(snaps * tiles * rows, LANES)
    own = pltpu.with_memory_space_constraint(own, pltpu.HBM)
    part = jax.ShapeDtypeStruct((own.shape[0] // cores, LANES), F32)
    keep, send = pl.pallas_call(
        functools.partial(pick_kernel, rows),
        out_shape=(part, part),
        in_specs=[HBM],
        out_specs=(VMEM, VMEM),
        scratch_shapes=[pltpu.VMEM(own.shape, F32), pltpu.SemaphoreType.DMA],
        compiler_params=PARAMS,
        cost_estimate=pl.CostEstimate(flops=10**9, bytes_accessed=own.size * 8, transcendentals=0),
        name="pick_rows",
    )(own)
    got = lax.ppermute(send, "grp", [(0, 1), (1, 0)])

    chunk = 6
    modes_panel, modes_gram = pl.pallas_call(
        modes_kernel,
        out_shape=(
            jax.ShapeDtypeStruct((2 * modes, slabs * LANES), BF16),
            jax.ShapeDtypeStruct((modes, modes), F32),
        ),
        in_specs=[VMEM],
        out_specs=(VMEM, VMEM),
        cost_estimate=pl.CostEstimate(flops=10**8, bytes_accessed=fields.size * 4, transcendentals=0),
        compiler_params=PARAMS,
        name="modes_gram",
    )(fields)
    snaps_panel, packed = pl.pallas_call(
        functools.partial(snaps_kernel, rows),
        out_shape=(
            jax.ShapeDtypeStruct((2 * snaps, slabs * LANES), BF16),
            jax.ShapeDtypeStruct((width // 2, LANES), F32),
        ),
        in_specs=[VMEM] * 4,
        out_specs=(VMEM, VMEM),
        compiler_params=PARAMS,
        cost_estimate=pl.CostEstimate(flops=10**8, bytes_accessed=10**6, transcendentals=0),
        name="snaps_gram",
    )(keep, got, modes_panel, modes_gram)
    packed = total(packed)
    scale = jnp.concatenate([weights, jnp.ones((snaps,), F32)])
    new_modes, factor = pl.pallas_call(
        functools.partial(apply_kernel, cells),
        out_shape=(
            jax.ShapeDtypeStruct((width, slabs, LANES), F32),
            jax.ShapeDtypeStruct((width, width), F32),
        ),
        in_specs=[VMEM] * 4,
        out_specs=(ANY, VMEM),
        scratch_shapes=[
            pltpu.VMEM((width, LANES), F32),
            pltpu.VMEM((width, slabs, LANES), F32),
            pltpu.SemaphoreType.DMA((chunk,)),
            *(pltpu.VMEM((n, TILE * TILE, LANES), F32) for n in (width // TILE, 2, 2, width // TILE)),
        ],
        compiler_params=PARAMS,
        name="factor_apply",
    )(packed, scale[:, None], modes_panel, snaps_panel)
    new_modes = new_modes.reshape(width, tiles, rows, LANES).transpose(0, 2, 1, 3)
    return new_modes.reshape(width, rows, cols), factor


def solution(mesh):
    in_specs = (P(None, AXES, None), P(), P(None, "srv", "grp"))
    out_specs = (P(None, AXES, None), P())
    return jax.shard_map(
        per_device, mesh=mesh, in_specs=in_specs, out_specs=out_specs, check_vma=False
    )
```

```python
import functools
import jax
import jax.numpy as jnp
from jax import lax
from jax.experimental.layout import Layout, with_layout_constraint
from jax.experimental import pallas as pl
from jax.experimental.pallas import tpu as pltpu
from jax.sharding import PartitionSpec as P

AXES = ("srv", "grp")
LANES = 128
TILE = 8
BLOCK = 16
F32, BF16 = jnp.float32, jnp.bfloat16
VMEM = pl.BlockSpec(memory_space=pltpu.VMEM)
ANY = pl.BlockSpec(memory_space=pl.ANY)
HBM = pl.BlockSpec(memory_space=pltpu.HBM)
PARAMS = pltpu.CompilerParams(vmem_limit_bytes=16 * 2**20)


def total(value):
    servers, cores = lax.axis_size("srv"), lax.axis_size("grp")
    if servers & (servers - 1) or cores != 2:
        return lax.psum(value, AXES)
    count = servers * cores
    masks = [1] + [2 * bit + 1 for bit in (1 << p for p in range(servers.bit_length() - 1))]
    for mask in masks:
        value = value + lax.ppermute(value, AXES, [(i, i ^ mask) for i in range(count)])
    return value


def packing(width):
    groups = []
    for r in reversed(range(width // BLOCK)):
        for group in groups:
            if sum(q + 1 for q in group) + r + 1 <= LANES // BLOCK:
                group.append(r)
                break
        else:
            groups.append([r])
    return groups


def split(x):
    high = x.astype(BF16)
    return high, (x - high.astype(F32)).astype(BF16)


def rows_times_rows(a, b):
    return lax.dot_general(a, b, (((1,), (1,)), ((), ())), preferred_element_type=F32)


def modes_kernel(modes, panel, gram):
    count = gram.shape[0]
    slabs = modes.shape[0] // count
    for i in range(slabs):
        high, low = split(modes[pl.ds(i, count, stride=slabs), :])
        panel[:count, i * LANES:(i + 1) * LANES] = high
        panel[count:, i * LANES:(i + 1) * LANES] = low
    acc = rows_times_rows(panel[...], panel[:count])
    cross = acc[count:]
    gram[...] = acc[:count] + cross + cross.T


def pick_kernel(rows, source, keep, send, snaps, sem):
    copy = pltpu.make_async_copy(source, snaps, sem)
    copy.start()
    copy.wait()
    core = lax.axis_index("grp")
    count = keep.shape[0] // rows
    stride = snaps.shape[0] // count
    for r in range(rows):
        at = slice(r * count, (r + 1) * count)
        keep[at] = snaps[pl.ds(core * rows + r, count, stride=stride), :]
        send[at] = snaps[pl.ds((1 - core) * rows + r, count, stride=stride), :]


def snaps_kernel(rows, keep, got, modes_panel, modes_gram, panel, packed):
    snaps, modes = panel.shape[0] // 2, modes_gram.shape[0]
    tiles = keep.shape[0] // (snaps * rows)
    kept = [lax.axis_index("grp") == h for h in (0, 1)]
    for h in (0, 1):
        for i in range(tiles * rows):
            place = pl.ds((i % rows) * snaps * tiles + i // rows, snaps, stride=tiles)
            high, low = split(jnp.where(kept[h], keep[place, :], got[place, :]))
            at = (h * tiles * rows + i) * LANES
            panel[:snaps, at:at + LANES] = high
            panel[snaps:, at:at + LANES] = low
    with_modes = rows_times_rows(modes_panel[...], panel[...])
    own = rows_times_rows(panel[...], panel[:snaps])
    top = with_modes[:modes]
    low_row = (top[:, :snaps] + top[:, snaps:] + with_modes[modes:, :snaps]).T
    own = own[:snaps] + own[snaps:] + own[snaps:].T
    whole = jnp.concatenate(
        [
            jnp.concatenate([modes_gram[...], jnp.zeros((modes, snaps), F32)], axis=1),
            jnp.concatenate([low_row, own], axis=1),
        ],
        axis=0,
    )
    for g, group in enumerate(packing(modes + snaps)):
        parts = [whole[r * BLOCK:(r + 1) * BLOCK, :(r + 1) * BLOCK] for r in group]
        spare = LANES - sum(p.shape[1] for p in parts)
        if spare:
            parts.append(jnp.zeros((BLOCK, spare), F32))
        packed[g * BLOCK:(g + 1) * BLOCK, :] = jnp.concatenate(parts, axis=1)


def spread_row(x, i):
    return jnp.broadcast_to(x[i:i + 1, :], (TILE, LANES))


def spread_column(x, j):
    return jnp.broadcast_to(x[:, j:j + 1], (x.shape[0], LANES))


def total_of(terms):
    terms = list(terms)
    while len(terms) > 1:
        terms = [sum(terms[i:i + 2]) for i in range(0, len(terms), 2)]
    return terms[0]


def everywhere(ref, row):
    return jnp.broadcast_to(ref[row:row + 1, :], (TILE, LANES))


def block_inverse(a):
    a = dict(a)
    l, m = {}, {}
    for p in range(0, TILE, 2):
        q = p + 1
        root = lax.rsqrt(a[p, p])
        det = a[p, p] * a[q, q] - a[q, p] * a[q, p]
        root_det = lax.rsqrt(det)
        over_det = root_det * root_det
        m[p, p] = root
        m[q, q] = root_det * (a[p, p] * root)
        l[q, p] = a[q, p] * root
        both = root_det * root
        w, z = {}, {}
        for i in range(q + 1, TILE):
            w[i] = a[p, p] * a[i, q] - a[q, p] * a[i, p]
            z[i] = a[q, q] * a[i, p] - a[q, p] * a[i, q]
            l[i, p] = a[i, p] * root
            l[i, q] = w[i] * both
        for k in range(q + 1, TILE):
            for i in range(k, TILE):
                a[i, k] = a[i, k] - (a[i, p] * z[k] + a[i, q] * w[k]) * over_det
        for i in (p, q):
            for k in range(i):
                m[i, k] = -m[i, i] * total_of(l[i, j] * m[j, k] for j in range(k, i))
    return m


def factor_tiles(tiles, entries, columns_of, rows_of, solved_of):
    count = len(tiles)
    lane = lax.broadcasted_iota(jnp.int32, (TILE, LANES), 1)
    tiles = list(tiles)
    upper, inverse = [], []
    square = TILE * TILE
    for b in range(2):
        columns_of[b] = jnp.zeros((square, LANES), F32)
        rows_of[b] = jnp.zeros((square, LANES), F32)
    diagonal = [spread_column(tiles[0], j) for j in range(TILE)]
    below = [[spread_column(x, j) for j in range(TILE)] for x in tiles[1:]]
    following = [spread_column(tiles[1], TILE + j) for j in range(TILE)]
    for t in range(count):
        at = t * TILE
        slot = entries.at[t]
        for j in range(TILE):
            slot[j * TILE:(j + 1) * TILE, :] = diagonal[j]
        m = block_inverse(
            {(i, j): everywhere(slot, j * TILE + i) for j in range(TILE) for i in range(j, TILE)}
        )
        if t + 1 < count:
            ahead = solved_of.at[t]
            for i in range(TILE):
                solved = total_of(m[i, j] * below[0][j] for j in range(i + 1))
                ahead[i * TILE:(i + 1) * TILE, :] = solved
            kept = [ahead[i * TILE:(i + 1) * TILE, :] for i in range(TILE)]
            diagonal = [
                following[k]
                - total_of(kept[i] * everywhere(ahead, i * TILE + k) for i in range(TILE))
                for k in range(TILE)
            ]
        by_column, by_row = columns_of.at[t % 2], rows_of.at[t % 2]
        for i in range(TILE):
            for k in range(i + 1):
                by_column[k * TILE + i:k * TILE + i + 1, :] = m[i, k][:1]
                by_row[i * TILE + k:i * TILE + k + 1, :] = m[i, k][:1]
        m_columns = [by_column[k * TILE:(k + 1) * TILE, :] for k in range(TILE)]
        row = total_of(m_columns[k] * spread_row(tiles[t], k) for k in range(TILE))
        block = (lane >= at) & (lane < at + TILE)
        mixed = row
        for k in range(TILE):
            mixed = jnp.where(lane == at + k, m_columns[k], mixed)
        upper.append(row)
        inverse.append(jnp.where(lane < at + TILE, mixed, 0.0))
        if t + 1 == count:
            break
        solved = total_of(
            by_row[i * TILE:(i + 1) * TILE, :] * spread_row(mixed, i) for i in range(TILE)
        )
        rows = [spread_row(solved, j) for j in range(TILE)]
        for s in range(t + 1, count):
            c = below[s - t - 1]
            tiles[s] = jnp.where(block, 0.0, tiles[s]) - total_of(c[j] * rows[j] for j in range(TILE))
        below = [[spread_column(x, at + TILE + j) for j in range(TILE)] for x in tiles[t + 2:]]
        if t + 2 < count:
            following = [spread_column(tiles[t + 2], at + 2 * TILE + j) for j in range(TILE)]
    return upper, inverse


def apply_kernel(cells, packed, scale, modes_panel, snaps_panel, out, factor, left, buf, lower_out, sems, *spread):
    modes, snaps = modes_panel.shape[0] // 2, snaps_panel.shape[0] // 2
    width = modes + snaps
    lane = lax.broadcasted_iota(jnp.int32, (BLOCK, LANES), 1)
    parts = {}
    for g, group in enumerate(packing(width)):
        strip = packed[g * BLOCK:(g + 1) * BLOCK, :] * (1.0 / cells)
        used = 0
        for r in group:
            piece = pltpu.roll(strip, LANES - used, 1) if used else strip
            parts[r] = jnp.where(lane < (r + 1) * BLOCK, piece, 0.0)
            used += (r + 1) * BLOCK
    lower = [parts[r] for r in range(width // BLOCK)] + [jnp.zeros((LANES - width, LANES), F32)]
    lower = jnp.concatenate(lower, axis=0)
    r = lax.broadcasted_iota(jnp.int32, (LANES, LANES), 0)
    c = lax.broadcasted_iota(jnp.int32, (LANES, LANES), 1)
    full = jnp.where(r >= c, lower, lower.T)
    upper, inverse = factor_tiles([full[i:i + TILE] for i in range(0, width, TILE)], *spread)
    for i, x in enumerate(inverse):
        left[i * TILE:(i + 1) * TILE, :] = x
    whole = jnp.concatenate(upper + [jnp.zeros((LANES - width, LANES), F32)], axis=0).T
    whole = jnp.where(r >= c, whole, 0.0)[:width, :width]
    lower_out[...] = whole * scale[...]
    chunks = sems.shape[0] - 1
    copies = [pltpu.make_async_copy(lower_out, factor, sems.at[chunks])]
    copies[0].start()
    w_high, w_low = split(left[:, :width])
    wm = jnp.concatenate([w_high[:, :modes], w_low[:, :modes]], axis=0)
    ws = jnp.concatenate([w_high[:, modes:], w_low[:, modes:]], axis=0)
    both_w = jnp.concatenate([wm, wm, ws, ws], axis=1)
    slabs = buf.shape[1]
    flat = buf.reshape(width * slabs, LANES)
    step = slabs // chunks
    for k in range(chunks):
        cols = slice(k * step * LANES, (k + 1) * step * LANES)
        right = jnp.concatenate([modes_panel[:, cols], snaps_panel[:, cols]], axis=0)
        res = jnp.dot(both_w, right, preferred_element_type=F32)
        res = res[:width] + res[width:]
        for i in range(step):
            flat[pl.ds(k * step + i, width, stride=slabs), :] = res[:, i * LANES:(i + 1) * LANES]
        part = (slice(None), pl.ds(k * step, step))
        copies.append(pltpu.make_async_copy(buf.at[part], out.at[part], sems.at[k]))
        copies[-1].start()
    for copy in copies:
        copy.wait()


def per_device(basis_modes, weights, snapshots):
    modes, rows, cols = basis_modes.shape
    snaps = snapshots.shape[0]
    width = modes + snaps
    tiles = cols // LANES
    slabs = rows * tiles
    cores = lax.axis_size("grp")
    cells = rows * cols * lax.axis_size("srv") * cores
    fields = basis_modes.reshape(modes, rows, tiles, LANES).transpose(0, 2, 1, 3)
    fields = fields.reshape(modes * slabs, LANES)
    own = snapshots.reshape(snaps, cores * rows, tiles // cores, LANES)
    own = with_layout_constraint(own, Layout((0, 2, 1, 3))).transpose(0, 2, 1, 3)
    own = own.reshape(snaps * tiles * rows, LANES)
    own = pltpu.with_memory_space_constraint(own, pltpu.HBM)
    part = jax.ShapeDtypeStruct((own.shape[0] // cores, LANES), F32)
    keep, send = pl.pallas_call(
        functools.partial(pick_kernel, rows),
        out_shape=(part, part),
        in_specs=[HBM],
        out_specs=(VMEM, VMEM),
        scratch_shapes=[pltpu.VMEM(own.shape, F32), pltpu.SemaphoreType.DMA],
        compiler_params=PARAMS,
        cost_estimate=pl.CostEstimate(flops=10**9, bytes_accessed=own.size * 8, transcendentals=0),
        name="pick_rows",
    )(own)
    got = lax.ppermute(send, "grp", [(0, 1), (1, 0)])

    chunk = 6
    modes_panel, modes_gram = pl.pallas_call(
        modes_kernel,
        out_shape=(
            jax.ShapeDtypeStruct((2 * modes, slabs * LANES), BF16),
            jax.ShapeDtypeStruct((modes, modes), F32),
        ),
        in_specs=[VMEM],
        out_specs=(VMEM, VMEM),
        cost_estimate=pl.CostEstimate(flops=10**8, bytes_accessed=fields.size * 4, transcendentals=0),
        compiler_params=PARAMS,
        name="modes_gram",
    )(fields)
    snaps_panel, packed = pl.pallas_call(
        functools.partial(snaps_kernel, rows),
        out_shape=(
            jax.ShapeDtypeStruct((2 * snaps, slabs * LANES), BF16),
            jax.ShapeDtypeStruct((len(packing(width)) * BLOCK, LANES), F32),
        ),
        in_specs=[VMEM] * 4,
        out_specs=(VMEM, VMEM),
        compiler_params=PARAMS,
        cost_estimate=pl.CostEstimate(flops=10**8, bytes_accessed=10**6, transcendentals=0),
        name="snaps_gram",
    )(keep, got, modes_panel, modes_gram)
    packed = total(packed)
    scale = jnp.concatenate([weights, jnp.ones((snaps,), F32)])
    new_modes, factor = pl.pallas_call(
        functools.partial(apply_kernel, cells),
        out_shape=(
            jax.ShapeDtypeStruct((width, slabs, LANES), F32),
            jax.ShapeDtypeStruct((width, width), F32),
        ),
        in_specs=[VMEM] * 4,
        out_specs=(ANY, ANY),
        scratch_shapes=[
            pltpu.VMEM((width, LANES), F32),
            pltpu.VMEM((width, slabs, LANES), F32),
            pltpu.VMEM((width, width), F32),
            pltpu.SemaphoreType.DMA((chunk + 1,)),
            *(pltpu.VMEM((n, TILE * TILE, LANES), F32) for n in (width // TILE, 2, 2, width // TILE)),
        ],
        compiler_params=PARAMS,
        name="factor_apply",
    )(packed, scale[:, None], modes_panel, snaps_panel)
    new_modes = new_modes.reshape(width, tiles, rows, LANES).transpose(0, 2, 1, 3)
    return new_modes.reshape(width, rows, cols), factor


def solution(mesh):
    in_specs = (P(None, AXES, None), P(), P(None, "srv", "grp"))
    out_specs = (P(None, AXES, None), P())
    return jax.shard_map(
        per_device, mesh=mesh, in_specs=in_specs, out_specs=out_specs, check_vma=False
    )
```

```python
import functools
import jax
import jax.numpy as jnp
from jax import lax
from jax.experimental.layout import Layout, with_layout_constraint
from jax.experimental import pallas as pl
from jax.experimental.pallas import tpu as pltpu
from jax.sharding import PartitionSpec as P

AXES = ("srv", "grp")
LANES = 128
TILE = 8
BLOCK = 16
F32, BF16 = jnp.float32, jnp.bfloat16
VMEM = pl.BlockSpec(memory_space=pltpu.VMEM)
ANY = pl.BlockSpec(memory_space=pl.ANY)
HBM = pl.BlockSpec(memory_space=pltpu.HBM)
PARAMS = pltpu.CompilerParams(vmem_limit_bytes=16 * 2**20)


def total(value):
    servers, cores = lax.axis_size("srv"), lax.axis_size("grp")
    if servers & (servers - 1) or servers < 4 or cores != 2:
        return lax.psum(value, AXES)
    count = servers * cores
    masks = [2 << p | 1 for p in range(servers.bit_length() - 1)]
    rounds = [[1], [masks[0], masks[1], masks[0] | masks[1]]] + [[mask] for mask in masks[2:]]
    for masks in rounds:
        parts = [lax.ppermute(value, AXES, [(i, i ^ m) for i in range(count)]) for m in masks]
        for part in parts:
            value = value + part
    return value


def packing(width):
    groups = []
    for r in reversed(range(width // BLOCK)):
        for group in groups:
            if sum(q + 1 for q in group) + r + 1 <= LANES // BLOCK:
                group.append(r)
                break
        else:
            groups.append([r])
    return groups


def split(x):
    high = x.astype(BF16)
    return high, (x - high.astype(F32)).astype(BF16)


def rows_times_rows(a, b):
    return lax.dot_general(a, b, (((1,), (1,)), ((), ())), preferred_element_type=F32)


def modes_kernel(modes, panel, gram):
    count = gram.shape[1]
    slabs = modes.shape[0] // count
    for i in range(slabs):
        high, low = split(modes[pl.ds(i, count, stride=slabs), :])
        panel[:count, i * LANES:(i + 1) * LANES] = high
        panel[count:, i * LANES:(i + 1) * LANES] = low
    gram[...] = rows_times_rows(panel[...], panel[:count])


def pick_kernel(rows, source, keep, send, snaps, sem):
    copy = pltpu.make_async_copy(source, snaps, sem)
    copy.start()
    copy.wait()
    core = lax.axis_index("grp")
    count = keep.shape[0] // rows
    stride = snaps.shape[0] // count
    for r in range(rows):
        at = slice(r * count, (r + 1) * count)
        keep[at] = snaps[pl.ds(core * rows + r, count, stride=stride), :]
        send[at] = snaps[pl.ds((1 - core) * rows + r, count, stride=stride), :]


def snaps_kernel(rows, keep, got, modes_panel, modes_gram, panel, packed):
    snaps, modes = panel.shape[0] // 2, modes_gram.shape[1]
    tiles = keep.shape[0] // (snaps * rows)
    kept = [lax.axis_index("grp") == h for h in (0, 1)]
    for h in (0, 1):
        for i in range(tiles * rows):
            place = pl.ds((i % rows) * snaps * tiles + i // rows, snaps, stride=tiles)
            high, low = split(jnp.where(kept[h], keep[place, :], got[place, :]))
            at = (h * tiles * rows + i) * LANES
            panel[:snaps, at:at + LANES] = high
            panel[snaps:, at:at + LANES] = low
    high = jnp.concatenate([modes_panel[:modes], panel[:snaps]], axis=0)
    low = jnp.concatenate([modes_panel[modes:], panel[snaps:]], axis=0)
    both = rows_times_rows(panel[...], high)
    last = both[:snaps] + both[snaps:] + rows_times_rows(panel[:snaps], low)
    cross = modes_gram[modes:]
    whole = jnp.concatenate([modes_gram[:modes] + cross + cross.T, jnp.zeros((modes, snaps), F32)], axis=1)
    whole = jnp.concatenate([whole, last], axis=0)
    for g, group in enumerate(packing(modes + snaps)):
        parts = [whole[r * BLOCK:(r + 1) * BLOCK, :(r + 1) * BLOCK] for r in group]
        spare = LANES - sum(p.shape[1] for p in parts)
        if spare:
            parts.append(jnp.zeros((BLOCK, spare), F32))
        packed[g * BLOCK:(g + 1) * BLOCK, :] = jnp.concatenate(parts, axis=1)


def spread_row(x, i):
    return jnp.broadcast_to(x[i:i + 1, :], (TILE, LANES))


def spread_column(x, j):
    return jnp.broadcast_to(x[:, j:j + 1], (x.shape[0], LANES))


def total_of(terms):
    terms = list(terms)
    while len(terms) > 1:
        terms = [sum(terms[i:i + 2]) for i in range(0, len(terms), 2)]
    return terms[0]


def everywhere(ref, row):
    return jnp.broadcast_to(ref[row:row + 1, :], (TILE, LANES))


def block_inverse(a):
    a = dict(a)
    l, m = {}, {}
    for p in range(0, TILE, 2):
        q = p + 1
        root = lax.rsqrt(a[p, p])
        det = a[p, p] * a[q, q] - a[q, p] * a[q, p]
        root_det = lax.rsqrt(det)
        over_det = root_det * root_det
        m[p, p] = root
        m[q, q] = root_det * (a[p, p] * root)
        l[q, p] = a[q, p] * root
        both = root_det * root
        w, z = {}, {}
        for i in range(q + 1, TILE):
            w[i] = a[p, p] * a[i, q] - a[q, p] * a[i, p]
            z[i] = a[q, q] * a[i, p] - a[q, p] * a[i, q]
            l[i, p] = a[i, p] * root
            l[i, q] = w[i] * both
        for k in range(q + 1, TILE):
            for i in range(k, TILE):
                a[i, k] = a[i, k] - (a[i, p] * z[k] + a[i, q] * w[k]) * over_det
        for i in (p, q):
            for k in range(i):
                m[i, k] = -m[i, i] * total_of(l[i, j] * m[j, k] for j in range(k, i))
    return m


def factor_tiles(tiles, lower, entries, columns_of, rows_of, solved_of):
    count = len(tiles)
    lane = lax.broadcasted_iota(jnp.int32, (TILE, LANES), 1)
    tiles = list(tiles)
    upper, inverse = [], []
    square = TILE * TILE
    for b in range(2):
        columns_of[b] = jnp.zeros((square, LANES), F32)
        rows_of[b] = jnp.zeros((square, LANES), F32)
    diagonal = [spread_column(lower[0], j) for j in range(TILE)]
    below = [[spread_column(x, j) for j in range(TILE)] for x in lower[1:]]
    following = [spread_column(lower[1], TILE + j) for j in range(TILE)]
    for t in range(count):
        at = t * TILE
        slot = entries.at[t]
        for j in range(TILE):
            slot[j * TILE:(j + 1) * TILE, :] = diagonal[j]
        m = block_inverse(
            {(i, j): everywhere(slot, j * TILE + i) for j in range(TILE) for i in range(j, TILE)}
        )
        if t + 1 < count:
            ahead = solved_of.at[t]
            for i in range(TILE):
                solved = total_of(m[i, j] * below[0][j] for j in range(i + 1))
                ahead[i * TILE:(i + 1) * TILE, :] = solved
            kept = [ahead[i * TILE:(i + 1) * TILE, :] for i in range(TILE)]
            diagonal = [
                following[k]
                - total_of(kept[i] * everywhere(ahead, i * TILE + k) for i in range(TILE))
                for k in range(TILE)
            ]
        by_column, by_row = columns_of.at[t % 2], rows_of.at[t % 2]
        for i in range(TILE):
            for k in range(i + 1):
                by_column[k * TILE + i:k * TILE + i + 1, :] = m[i, k][:1]
                by_row[i * TILE + k:i * TILE + k + 1, :] = m[i, k][:1]
        m_columns = [by_column[k * TILE:(k + 1) * TILE, :] for k in range(TILE)]
        row = total_of(m_columns[k] * spread_row(tiles[t], k) for k in range(TILE))
        block = (lane >= at) & (lane < at + TILE)
        mixed = row
        for k in range(TILE):
            mixed = jnp.where(lane == at + k, m_columns[k], mixed)
        upper.append(row)
        inverse.append(jnp.where(lane < at + TILE, mixed, 0.0))
        if t + 1 == count:
            break
        solved = total_of(
            by_row[i * TILE:(i + 1) * TILE, :] * spread_row(mixed, i) for i in range(TILE)
        )
        rows = [spread_row(solved, j) for j in range(TILE)]
        for s in range(t + 1, count):
            c = below[s - t - 1]
            tiles[s] = jnp.where(block, 0.0, tiles[s]) - total_of(c[j] * rows[j] for j in range(TILE))
        below = [[spread_column(x, at + TILE + j) for j in range(TILE)] for x in tiles[t + 2:]]
        if t + 2 < count:
            following = [spread_column(tiles[t + 2], at + 2 * TILE + j) for j in range(TILE)]
    return upper, inverse


def apply_kernel(cells, packed, scale, modes_panel, snaps_panel, out, factor, buf, lower_out, sems, *spread):
    modes, snaps = modes_panel.shape[0] // 2, snaps_panel.shape[0] // 2
    width = modes + snaps
    lane = lax.broadcasted_iota(jnp.int32, (BLOCK, LANES), 1)
    parts = {}
    for g, group in enumerate(packing(width)):
        strip = packed[g * BLOCK:(g + 1) * BLOCK, :] * (1.0 / cells)
        used = 0
        for r in group:
            piece = pltpu.roll(strip, LANES - used, 1) if used else strip
            parts[r] = jnp.where(lane < (r + 1) * BLOCK, piece, 0.0)
            used += (r + 1) * BLOCK
    lower = [parts[r] for r in range(width // BLOCK)] + [jnp.zeros((LANES - width, LANES), F32)]
    lower = jnp.concatenate(lower, axis=0)
    r = lax.broadcasted_iota(jnp.int32, (LANES, LANES), 0)
    c = lax.broadcasted_iota(jnp.int32, (LANES, LANES), 1)
    full = jnp.where(r >= c, lower, lower.T)
    upper, inverse = factor_tiles(
        *([x[i:i + TILE] for i in range(0, width, TILE)] for x in (full, lower)), *spread
    )
    left = jnp.concatenate(inverse, axis=0)
    whole = jnp.concatenate(upper + [jnp.zeros((LANES - width, LANES), F32)], axis=0).T
    whole = jnp.where(r >= c, whole, 0.0)[:width, :width]
    lower_out[...] = whole * scale[...]
    chunks = sems.shape[0] - 1
    copies = [pltpu.make_async_copy(lower_out, factor, sems.at[chunks])]
    copies[0].start()
    w_high, w_low = split(left[:, :width])
    wm = jnp.concatenate([w_high[:, :modes], w_low[:, :modes]], axis=0)
    ws = jnp.concatenate([w_high[:, modes:], w_low[:, modes:]], axis=0)
    both_w = jnp.concatenate([wm, wm, ws, ws], axis=1)
    slabs = buf.shape[1]
    flat = buf.reshape(width * slabs, LANES)
    step = slabs // chunks
    for k in range(chunks):
        cols = slice(k * step * LANES, (k + 1) * step * LANES)
        right = jnp.concatenate([modes_panel[:, cols], snaps_panel[:, cols]], axis=0)
        res = jnp.dot(both_w, right, preferred_element_type=F32)
        res = res[:width] + res[width:]
        for i in range(step):
            flat[pl.ds(k * step + i, width, stride=slabs), :] = res[:, i * LANES:(i + 1) * LANES]
        part = (slice(None), pl.ds(k * step, step))
        copies.append(pltpu.make_async_copy(buf.at[part], out.at[part], sems.at[k]))
        copies[-1].start()
    for copy in copies:
        copy.wait()


def per_device(basis_modes, weights, snapshots):
    modes, rows, cols = basis_modes.shape
    snaps = snapshots.shape[0]
    width = modes + snaps
    tiles = cols // LANES
    slabs = rows * tiles
    cores = lax.axis_size("grp")
    cells = rows * cols * lax.axis_size("srv") * cores
    fields = basis_modes.reshape(modes, rows, tiles, LANES).transpose(0, 2, 1, 3)
    fields = fields.reshape(modes * slabs, LANES)
    own = snapshots.reshape(snaps, cores * rows, tiles // cores, LANES)
    own = with_layout_constraint(own, Layout((0, 2, 1, 3))).transpose(0, 2, 1, 3)
    own = own.reshape(snaps * tiles * rows, LANES)
    own = pltpu.with_memory_space_constraint(own, pltpu.HBM)
    part = jax.ShapeDtypeStruct((own.shape[0] // cores, LANES), F32)
    keep, send = pl.pallas_call(
        functools.partial(pick_kernel, rows),
        out_shape=(part, part),
        in_specs=[HBM],
        out_specs=(VMEM, VMEM),
        scratch_shapes=[pltpu.VMEM(own.shape, F32), pltpu.SemaphoreType.DMA],
        compiler_params=PARAMS,
        cost_estimate=pl.CostEstimate(flops=10**9, bytes_accessed=own.size * 8, transcendentals=0),
        name="pick_rows",
    )(own)
    got = lax.ppermute(send, "grp", [(0, 1), (1, 0)])

    chunk = 6
    modes_panel, modes_gram = pl.pallas_call(
        modes_kernel,
        out_shape=(
            jax.ShapeDtypeStruct((2 * modes, slabs * LANES), BF16),
            jax.ShapeDtypeStruct((2 * modes, modes), F32),
        ),
        in_specs=[VMEM],
        out_specs=(VMEM, VMEM),
        cost_estimate=pl.CostEstimate(flops=10**8, bytes_accessed=fields.size * 4, transcendentals=0),
        compiler_params=PARAMS,
        name="modes_gram",
    )(fields)
    snaps_panel, packed = pl.pallas_call(
        functools.partial(snaps_kernel, rows),
        out_shape=(
            jax.ShapeDtypeStruct((2 * snaps, slabs * LANES), BF16),
            jax.ShapeDtypeStruct((len(packing(width)) * BLOCK, LANES), F32),
        ),
        in_specs=[VMEM] * 4,
        out_specs=(VMEM, VMEM),
        compiler_params=PARAMS,
        cost_estimate=pl.CostEstimate(flops=10**8, bytes_accessed=10**6, transcendentals=0),
        name="snaps_gram",
    )(keep, got, modes_panel, modes_gram)
    packed = total(packed)
    scale = jnp.concatenate([weights, jnp.ones((snaps,), F32)])
    new_modes, factor = pl.pallas_call(
        functools.partial(apply_kernel, cells),
        out_shape=(
            jax.ShapeDtypeStruct((width, slabs, LANES), F32),
            jax.ShapeDtypeStruct((width, width), F32),
        ),
        in_specs=[VMEM] * 4,
        out_specs=(ANY, ANY),
        scratch_shapes=[
            pltpu.VMEM((width, slabs, LANES), F32),
            pltpu.VMEM((width, width), F32),
            pltpu.SemaphoreType.DMA((chunk + 1,)),
            *(pltpu.VMEM((n, TILE * TILE, LANES), F32) for n in (width // TILE, 2, 2, width // TILE)),
        ],
        compiler_params=PARAMS,
        name="factor_apply",
    )(packed, scale[:, None], modes_panel, snaps_panel)
    new_modes = new_modes.reshape(width, tiles, rows, LANES).transpose(0, 2, 1, 3)
    return new_modes.reshape(width, rows, cols), factor


def solution(mesh):
    in_specs = (P(None, AXES, None), P(), P(None, "srv", "grp"))
    out_specs = (P(None, AXES, None), P())
    return jax.shard_map(
        per_device, mesh=mesh, in_specs=in_specs, out_specs=out_specs, check_vma=False
    )
```

```python
import functools
import jax
import jax.numpy as jnp
from jax import lax
from jax.experimental.layout import Layout, with_layout_constraint
from jax.experimental import pallas as pl
from jax.experimental.pallas import tpu as pltpu
from jax.sharding import PartitionSpec as P

AXES = ("srv", "grp")
LANES = 128
TILE = 8
BLOCK = 16
PIECES = 2
F32, BF16 = jnp.float32, jnp.bfloat16
VMEM = pl.BlockSpec(memory_space=pltpu.VMEM)
ANY = pl.BlockSpec(memory_space=pl.ANY)
HBM = pl.BlockSpec(memory_space=pltpu.HBM)
PARAMS = pltpu.CompilerParams(vmem_limit_bytes=16 * 2**20)


def total(value):
    servers, cores = lax.axis_size("srv"), lax.axis_size("grp")
    if servers & (servers - 1) or servers < 4 or cores != 2:
        return lax.psum(value, AXES)
    count = servers * cores
    masks = [2 << p | 1 for p in range(servers.bit_length() - 1)]
    rounds = [[1], [masks[0], masks[1], masks[0] | masks[1]]] + [[mask] for mask in masks[2:]]
    for masks in rounds:
        parts = [lax.ppermute(value, AXES, [(i, i ^ m) for i in range(count)]) for m in masks]
        for part in parts:
            value = value + part
    return value


def packing(width):
    groups = []
    for r in reversed(range(width // BLOCK)):
        for group in groups:
            if sum(q + 1 for q in group) + r + 1 <= LANES // BLOCK:
                group.append(r)
                break
        else:
            groups.append([r])
    return groups


def split(x):
    high = x.astype(BF16)
    return high, (x - high.astype(F32)).astype(BF16)


def rows_times_rows(a, b):
    return lax.dot_general(a, b, (((1,), (1,)), ((), ())), preferred_element_type=F32)


def modes_kernel(source, panel, gram, buf, sems):
    count, slabs, _ = source.shape
    flat = buf.reshape(count * slabs, LANES)
    pieces = sems.shape[0]
    step = slabs // pieces
    copies = []
    for p in range(pieces):
        part = (slice(None), pl.ds(p * step, step))
        copies.append(pltpu.make_async_copy(source.at[part], buf.at[part], sems.at[p]))
        copies[-1].start()
    terms = []
    for p in range(pieces):
        copies[p].wait()
        for i in range(p * step, (p + 1) * step):
            high, low = split(flat[pl.ds(i, count, stride=slabs), :])
            panel[:count, i * LANES:(i + 1) * LANES] = high
            panel[count:, i * LANES:(i + 1) * LANES] = low
        cols = slice(p * step * LANES, (p + 1) * step * LANES)
        terms.append(rows_times_rows(panel[:, cols], panel[:count, cols]))
    gram[...] = total_of(terms)


def snaps_kernel(rows, keep, got, modes_panel, modes_gram, panel, packed):
    snaps, modes = panel.shape[0] // 2, modes_gram.shape[1]
    core = lax.axis_index("grp")
    stride = keep.shape[0] // snaps
    here = stride // 2
    for h in (0, 1):
        for i in range(here):
            start = i // rows * 2 * rows + core * rows + i % rows
            place = pl.ds(start, snaps, stride=stride)
            high, low = split(jnp.where(core == h, keep[place, :], got[place, :]))
            at = (h * here + i) * LANES
            panel[:snaps, at:at + LANES] = high
            panel[snaps:, at:at + LANES] = low
    high = jnp.concatenate([modes_panel[:modes], panel[:snaps]], axis=0)
    low = jnp.concatenate([modes_panel[modes:], panel[snaps:]], axis=0)
    both = rows_times_rows(panel[...], high)
    last = both[:snaps] + both[snaps:] + rows_times_rows(panel[:snaps], low)
    cross = modes_gram[modes:]
    whole = jnp.concatenate([modes_gram[:modes] + cross + cross.T, jnp.zeros((modes, snaps), F32)], axis=1)
    whole = jnp.concatenate([whole, last], axis=0)
    for g, group in enumerate(packing(modes + snaps)):
        parts = [whole[r * BLOCK:(r + 1) * BLOCK, :(r + 1) * BLOCK] for r in group]
        spare = LANES - sum(p.shape[1] for p in parts)
        if spare:
            parts.append(jnp.zeros((BLOCK, spare), F32))
        packed[g * BLOCK:(g + 1) * BLOCK, :] = jnp.concatenate(parts, axis=1)


def spread_row(x, i):
    return jnp.broadcast_to(x[i:i + 1, :], (TILE, LANES))


def spread_column(x, j):
    return jnp.broadcast_to(x[:, j:j + 1], (x.shape[0], LANES))


def total_of(terms):
    terms = list(terms)
    while len(terms) > 1:
        terms = [sum(terms[i:i + 2]) for i in range(0, len(terms), 2)]
    return terms[0]


def everywhere(ref, row):
    return jnp.broadcast_to(ref[row:row + 1, :], (TILE, LANES))


def block_inverse(a):
    a = dict(a)
    l, m = {}, {}
    for p in range(0, TILE, 2):
        q = p + 1
        root = lax.rsqrt(a[p, p])
        det = a[p, p] * a[q, q] - a[q, p] * a[q, p]
        root_det = lax.rsqrt(det)
        over_det = root_det * root_det
        m[p, p] = root
        m[q, q] = root_det * (a[p, p] * root)
        l[q, p] = a[q, p] * root
        both = root_det * root
        w, z = {}, {}
        for i in range(q + 1, TILE):
            w[i] = a[p, p] * a[i, q] - a[q, p] * a[i, p]
            z[i] = a[q, q] * a[i, p] - a[q, p] * a[i, q]
            l[i, p] = a[i, p] * root
            l[i, q] = w[i] * both
        for k in range(q + 1, TILE):
            for i in range(k, TILE):
                a[i, k] = a[i, k] - (a[i, p] * z[k] + a[i, q] * w[k]) * over_det
        for i in (p, q):
            for k in range(i):
                m[i, k] = -m[i, i] * total_of(l[i, j] * m[j, k] for j in range(k, i))
    return m


def factor_tiles(tiles, lower, entries, columns_of, rows_of, solved_of):
    count = len(tiles)
    lane = lax.broadcasted_iota(jnp.int32, (TILE, LANES), 1)
    tiles = list(tiles)
    upper, inverse = [], []
    square = TILE * TILE
    for b in range(2):
        columns_of[b] = jnp.zeros((square, LANES), F32)
        rows_of[b] = jnp.zeros((square, LANES), F32)
    diagonal = [spread_column(lower[0], j) for j in range(TILE)]
    below = [[spread_column(x, j) for j in range(TILE)] for x in lower[1:]]
    following = [spread_column(lower[1], TILE + j) for j in range(TILE)]
    for t in range(count):
        at = t * TILE
        slot = entries.at[t]
        for j in range(TILE):
            slot[j * TILE:(j + 1) * TILE, :] = diagonal[j]
        m = block_inverse(
            {(i, j): everywhere(slot, j * TILE + i) for j in range(TILE) for i in range(j, TILE)}
        )
        if t + 1 < count:
            ahead = solved_of.at[t]
            for i in range(TILE):
                solved = total_of(m[i, j] * below[0][j] for j in range(i + 1))
                ahead[i * TILE:(i + 1) * TILE, :] = solved
            kept = [ahead[i * TILE:(i + 1) * TILE, :] for i in range(TILE)]
            diagonal = [
                following[k]
                - total_of(kept[i] * everywhere(ahead, i * TILE + k) for i in range(TILE))
                for k in range(TILE)
            ]
        by_column, by_row = columns_of.at[t % 2], rows_of.at[t % 2]
        for i in range(TILE):
            for k in range(i + 1):
                by_column[k * TILE + i:k * TILE + i + 1, :] = m[i, k][:1]
                by_row[i * TILE + k:i * TILE + k + 1, :] = m[i, k][:1]
        m_columns = [by_column[k * TILE:(k + 1) * TILE, :] for k in range(TILE)]
        row = total_of(m_columns[k] * spread_row(tiles[t], k) for k in range(TILE))
        block = (lane >= at) & (lane < at + TILE)
        mixed = row
        for k in range(TILE):
            mixed = jnp.where(lane == at + k, m_columns[k], mixed)
        upper.append(row)
        inverse.append(jnp.where(lane < at + TILE, mixed, 0.0))
        if t + 1 == count:
            break
        solved = total_of(
            by_row[i * TILE:(i + 1) * TILE, :] * spread_row(mixed, i) for i in range(TILE)
        )
        rows = [spread_row(solved, j) for j in range(TILE)]
        for s in range(t + 1, count):
            c = below[s - t - 1]
            tiles[s] = jnp.where(block, 0.0, tiles[s]) - total_of(c[j] * rows[j] for j in range(TILE))
        below = [[spread_column(x, at + TILE + j) for j in range(TILE)] for x in tiles[t + 2:]]
        if t + 2 < count:
            following = [spread_column(tiles[t + 2], at + 2 * TILE + j) for j in range(TILE)]
    return upper, inverse


def apply_kernel(cells, packed, scale, modes_panel, snaps_panel, out, factor, buf, lower_out, sems, *spread):
    modes, snaps = modes_panel.shape[0] // 2, snaps_panel.shape[0] // 2
    width = modes + snaps
    lane = lax.broadcasted_iota(jnp.int32, (BLOCK, LANES), 1)
    parts = {}
    for g, group in enumerate(packing(width)):
        strip = packed[g * BLOCK:(g + 1) * BLOCK, :] * (1.0 / cells)
        used = 0
        for r in group:
            piece = pltpu.roll(strip, LANES - used, 1) if used else strip
            parts[r] = jnp.where(lane < (r + 1) * BLOCK, piece, 0.0)
            used += (r + 1) * BLOCK
    lower = [parts[r] for r in range(width // BLOCK)] + [jnp.zeros((LANES - width, LANES), F32)]
    lower = jnp.concatenate(lower, axis=0)
    r = lax.broadcasted_iota(jnp.int32, (LANES, LANES), 0)
    c = lax.broadcasted_iota(jnp.int32, (LANES, LANES), 1)
    full = jnp.where(r >= c, lower, lower.T)
    upper, inverse = factor_tiles(
        *([x[i:i + TILE] for i in range(0, width, TILE)] for x in (full, lower)), *spread
    )
    left = jnp.concatenate(inverse, axis=0)
    whole = jnp.concatenate(upper + [jnp.zeros((LANES - width, LANES), F32)], axis=0).T
    whole = jnp.where(r >= c, whole, 0.0)[:width, :width]
    lower_out[...] = whole * scale[...]
    chunks = sems.shape[0] - 1
    copies = [pltpu.make_async_copy(lower_out, factor, sems.at[chunks])]
    copies[0].start()
    w_high, w_low = split(left[:, :width])
    wm = jnp.concatenate([w_high[:, :modes], w_low[:, :modes]], axis=0)
    ws = jnp.concatenate([w_high[:, modes:], w_low[:, modes:]], axis=0)
    both_w = jnp.concatenate([wm, wm, ws, ws], axis=1)
    slabs = buf.shape[1]
    flat = buf.reshape(width * slabs, LANES)
    step = slabs // chunks
    for k in range(chunks):
        cols = slice(k * step * LANES, (k + 1) * step * LANES)
        right = jnp.concatenate([modes_panel[:, cols], snaps_panel[:, cols]], axis=0)
        res = jnp.dot(both_w, right, preferred_element_type=F32)
        res = res[:width] + res[width:]
        for i in range(step):
            flat[pl.ds(k * step + i, width, stride=slabs), :] = res[:, i * LANES:(i + 1) * LANES]
        part = (slice(None), pl.ds(k * step, step))
        copies.append(pltpu.make_async_copy(buf.at[part], out.at[part], sems.at[k]))
        copies[-1].start()
    for copy in copies:
        copy.wait()


def per_device(basis_modes, weights, snapshots):
    modes, rows, cols = basis_modes.shape
    snaps = snapshots.shape[0]
    width = modes + snaps
    tiles = cols // LANES
    slabs = rows * tiles
    cores = lax.axis_size("grp")
    cells = rows * cols * lax.axis_size("srv") * cores
    fields = basis_modes.reshape(modes, rows, tiles, LANES).transpose(0, 2, 1, 3)
    fields = pltpu.with_memory_space_constraint(fields.reshape(modes, slabs, LANES), pltpu.HBM)
    own = snapshots.reshape(snaps, cores * rows, tiles // cores, LANES)
    own = with_layout_constraint(own, Layout((0, 2, 1, 3))).transpose(0, 2, 1, 3)
    own = own.reshape(snaps * tiles * rows, LANES)
    got = lax.ppermute(own, "grp", [(0, 1), (1, 0)])

    chunk = 6
    modes_panel, modes_gram = pl.pallas_call(
        modes_kernel,
        out_shape=(
            jax.ShapeDtypeStruct((2 * modes, slabs * LANES), BF16),
            jax.ShapeDtypeStruct((2 * modes, modes), F32),
        ),
        in_specs=[HBM],
        out_specs=(VMEM, VMEM),
        scratch_shapes=[pltpu.VMEM(fields.shape, F32), pltpu.SemaphoreType.DMA((PIECES,))],
        cost_estimate=pl.CostEstimate(flops=10**8, bytes_accessed=fields.size * 4, transcendentals=0),
        compiler_params=PARAMS,
        name="modes_gram",
    )(fields)
    snaps_panel, packed = pl.pallas_call(
        functools.partial(snaps_kernel, rows),
        out_shape=(
            jax.ShapeDtypeStruct((2 * snaps, slabs * LANES), BF16),
            jax.ShapeDtypeStruct((len(packing(width)) * BLOCK, LANES), F32),
        ),
        in_specs=[VMEM] * 4,
        out_specs=(VMEM, VMEM),
        compiler_params=PARAMS,
        cost_estimate=pl.CostEstimate(flops=10**8, bytes_accessed=10**6, transcendentals=0),
        name="snaps_gram",
    )(own, got, modes_panel, modes_gram)
    packed = total(packed)
    scale = jnp.concatenate([weights, jnp.ones((snaps,), F32)])
    new_modes, factor = pl.pallas_call(
        functools.partial(apply_kernel, cells),
        out_shape=(
            jax.ShapeDtypeStruct((width, slabs, LANES), F32),
            jax.ShapeDtypeStruct((width, width), F32),
        ),
        in_specs=[VMEM] * 4,
        out_specs=(ANY, ANY),
        scratch_shapes=[
            pltpu.VMEM((width, slabs, LANES), F32),
            pltpu.VMEM((width, width), F32),
            pltpu.SemaphoreType.DMA((chunk + 1,)),
            *(pltpu.VMEM((n, TILE * TILE, LANES), F32) for n in (width // TILE, 2, 2, width // TILE)),
        ],
        compiler_params=PARAMS,
        name="factor_apply",
    )(packed, scale[:, None], modes_panel, snaps_panel)
    new_modes = new_modes.reshape(width, tiles, rows, LANES).transpose(0, 2, 1, 3)
    return new_modes.reshape(width, rows, cols), factor


def solution(mesh):
    in_specs = (P(None, AXES, None), P(), P(None, "srv", "grp"))
    out_specs = (P(None, AXES, None), P())
    return jax.shard_map(
        per_device, mesh=mesh, in_specs=in_specs, out_specs=out_specs, check_vma=False
    )
```

```python
import functools
import jax
import jax.numpy as jnp
from jax import lax
from jax.experimental.layout import Layout, with_layout_constraint
from jax.experimental import pallas as pl
from jax.experimental.pallas import tpu as pltpu
from jax.sharding import PartitionSpec as P

AXES = ("srv", "grp")
LANES = 128
TILE = 8
BLOCK = 16
COST = 10**9
F32, BF16 = jnp.float32, jnp.bfloat16
VMEM = pl.BlockSpec(memory_space=pltpu.VMEM)
ANY = pl.BlockSpec(memory_space=pl.ANY)
HBM = pl.BlockSpec(memory_space=pltpu.HBM)
PARAMS = pltpu.CompilerParams(vmem_limit_bytes=16 * 2**20)


def total(value):
    servers, cores = lax.axis_size("srv"), lax.axis_size("grp")
    if servers & (servers - 1) or servers < 4 or cores != 2:
        return lax.psum(value, AXES)
    count = servers * cores
    masks = [2 << p | 1 for p in range(servers.bit_length() - 1)]
    rounds = [[1], [masks[0], masks[1], masks[0] | masks[1]]] + [[mask] for mask in masks[2:]]
    for masks in rounds:
        parts = [lax.ppermute(value, AXES, [(i, i ^ m) for i in range(count)]) for m in masks]
        for part in parts:
            value = value + part
    return value


def packing(width):
    groups = []
    for r in reversed(range(width // BLOCK)):
        for group in groups:
            if sum(q + 1 for q in group) + r + 1 <= LANES // BLOCK:
                group.append(r)
                break
        else:
            groups.append([r])
    return groups


def split(x):
    high = x.astype(BF16)
    return high, (x - high.astype(F32)).astype(BF16)


def rows_times_rows(a, b):
    return lax.dot_general(a, b, (((1,), (1,)), ((), ())), preferred_element_type=F32)


def ones_kernel(out):
    out[...] = jnp.ones(out.shape, F32)


def modes_kernel(modes, panel, gram):
    count = gram.shape[1]
    slabs = modes.shape[0] // count
    for i in range(slabs):
        high, low = split(modes[pl.ds(i, count, stride=slabs), :])
        panel[:count, i * LANES:(i + 1) * LANES] = high
        panel[count:, i * LANES:(i + 1) * LANES] = low
    gram[...] = rows_times_rows(panel[...], panel[:count])


def snaps_kernel(rows, keep, got, modes_panel, modes_gram, panel, packed):
    snaps, modes = panel.shape[0] // 2, modes_gram.shape[1]
    core = lax.axis_index("grp")
    stride = keep.shape[0] // snaps
    here = stride // 2
    for h in (0, 1):
        for i in range(here):
            start = i // rows * 2 * rows + core * rows + i % rows
            place = pl.ds(start, snaps, stride=stride)
            high, low = split(jnp.where(core == h, keep[place, :], got[place, :]))
            at = (h * here + i) * LANES
            panel[:snaps, at:at + LANES] = high
            panel[snaps:, at:at + LANES] = low
    high = jnp.concatenate([modes_panel[:modes], panel[:snaps]], axis=0)
    low = jnp.concatenate([modes_panel[modes:], panel[snaps:]], axis=0)
    both = rows_times_rows(panel[...], high)
    last = both[:snaps] + both[snaps:] + rows_times_rows(panel[:snaps], low)
    cross = modes_gram[modes:]
    whole = jnp.concatenate([modes_gram[:modes] + cross + cross.T, jnp.zeros((modes, snaps), F32)], axis=1)
    whole = jnp.concatenate([whole, last], axis=0)
    for g, group in enumerate(packing(modes + snaps)):
        parts = [whole[r * BLOCK:(r + 1) * BLOCK, :(r + 1) * BLOCK] for r in group]
        spare = LANES - sum(p.shape[1] for p in parts)
        if spare:
            parts.append(jnp.zeros((BLOCK, spare), F32))
        packed[g * BLOCK:(g + 1) * BLOCK, :] = jnp.concatenate(parts, axis=1)


def spread_row(x, i):
    return jnp.broadcast_to(x[i:i + 1, :], (TILE, LANES))


def spread_column(x, j):
    return jnp.broadcast_to(x[:, j:j + 1], (x.shape[0], LANES))


def total_of(terms):
    terms = list(terms)
    while len(terms) > 1:
        terms = [sum(terms[i:i + 2]) for i in range(0, len(terms), 2)]
    return terms[0]


def everywhere(ref, row):
    return jnp.broadcast_to(ref[row:row + 1, :], (TILE, LANES))


def block_inverse(a):
    a = dict(a)
    l, m = {}, {}
    for p in range(0, TILE, 2):
        q = p + 1
        root = lax.rsqrt(a[p, p])
        det = a[p, p] * a[q, q] - a[q, p] * a[q, p]
        root_det = lax.rsqrt(det)
        over_det = root_det * root_det
        m[p, p] = root
        m[q, q] = root_det * (a[p, p] * root)
        l[q, p] = a[q, p] * root
        both = root_det * root
        w, z = {}, {}
        for i in range(q + 1, TILE):
            w[i] = a[p, p] * a[i, q] - a[q, p] * a[i, p]
            z[i] = a[q, q] * a[i, p] - a[q, p] * a[i, q]
            l[i, p] = a[i, p] * root
            l[i, q] = w[i] * both
        for k in range(q + 1, TILE):
            for i in range(k, TILE):
                a[i, k] = a[i, k] - (a[i, p] * z[k] + a[i, q] * w[k]) * over_det
        for i in (p, q):
            for k in range(i):
                m[i, k] = -m[i, i] * total_of(l[i, j] * m[j, k] for j in range(k, i))
    return m


def factor_tiles(tiles, lower, entries, columns_of, rows_of, solved_of):
    count = len(tiles)
    lane = lax.broadcasted_iota(jnp.int32, (TILE, LANES), 1)
    tiles = list(tiles)
    upper, inverse = [], []
    square = TILE * TILE
    for b in range(2):
        columns_of[b] = jnp.zeros((square, LANES), F32)
        rows_of[b] = jnp.zeros((square, LANES), F32)
    diagonal = [spread_column(lower[0], j) for j in range(TILE)]
    below = [[spread_column(x, j) for j in range(TILE)] for x in lower[1:]]
    following = [spread_column(lower[1], TILE + j) for j in range(TILE)]
    for t in range(count):
        at = t * TILE
        slot = entries.at[t]
        for j in range(TILE):
            slot[j * TILE:(j + 1) * TILE, :] = diagonal[j]
        m = block_inverse(
            {(i, j): everywhere(slot, j * TILE + i) for j in range(TILE) for i in range(j, TILE)}
        )
        if t + 1 < count:
            ahead = solved_of.at[t]
            for i in range(TILE):
                solved = total_of(m[i, j] * below[0][j] for j in range(i + 1))
                ahead[i * TILE:(i + 1) * TILE, :] = solved
            kept = [ahead[i * TILE:(i + 1) * TILE, :] for i in range(TILE)]
            diagonal = [
                following[k]
                - total_of(kept[i] * everywhere(ahead, i * TILE + k) for i in range(TILE))
                for k in range(TILE)
            ]
        by_column, by_row = columns_of.at[t % 2], rows_of.at[t % 2]
        for i in range(TILE):
            for k in range(i + 1):
                by_column[k * TILE + i:k * TILE + i + 1, :] = m[i, k][:1]
                by_row[i * TILE + k:i * TILE + k + 1, :] = m[i, k][:1]
        m_columns = [by_column[k * TILE:(k + 1) * TILE, :] for k in range(TILE)]
        row = total_of(m_columns[k] * spread_row(tiles[t], k) for k in range(TILE))
        block = (lane >= at) & (lane < at + TILE)
        mixed = row
        for k in range(TILE):
            mixed = jnp.where(lane == at + k, m_columns[k], mixed)
        upper.append(row)
        inverse.append(jnp.where(lane < at + TILE, mixed, 0.0))
        if t + 1 == count:
            break
        solved = total_of(
            by_row[i * TILE:(i + 1) * TILE, :] * spread_row(mixed, i) for i in range(TILE)
        )
        rows = [spread_row(solved, j) for j in range(TILE)]
        for s in range(t + 1, count):
            c = below[s - t - 1]
            tiles[s] = jnp.where(block, 0.0, tiles[s]) - total_of(c[j] * rows[j] for j in range(TILE))
        below = [[spread_column(x, at + TILE + j) for j in range(TILE)] for x in tiles[t + 2:]]
        if t + 2 < count:
            following = [spread_column(tiles[t + 2], at + 2 * TILE + j) for j in range(TILE)]
    return upper, inverse


def apply_kernel(cells, packed, scale, modes_panel, snaps_panel, out, factor, buf, lower_out, sems, *spread):
    modes, snaps = modes_panel.shape[0] // 2, snaps_panel.shape[0] // 2
    width = modes + snaps
    lane = lax.broadcasted_iota(jnp.int32, (BLOCK, LANES), 1)
    parts = {}
    for g, group in enumerate(packing(width)):
        strip = packed[g * BLOCK:(g + 1) * BLOCK, :] * (1.0 / cells)
        used = 0
        for r in group:
            piece = pltpu.roll(strip, LANES - used, 1) if used else strip
            parts[r] = jnp.where(lane < (r + 1) * BLOCK, piece, 0.0)
            used += (r + 1) * BLOCK
    lower = [parts[r] for r in range(width // BLOCK)] + [jnp.zeros((LANES - width, LANES), F32)]
    lower = jnp.concatenate(lower, axis=0)
    r = lax.broadcasted_iota(jnp.int32, (LANES, LANES), 0)
    c = lax.broadcasted_iota(jnp.int32, (LANES, LANES), 1)
    full = jnp.where(r >= c, lower, lower.T)
    upper, inverse = factor_tiles(
        *([x[i:i + TILE] for i in range(0, width, TILE)] for x in (full, lower)), *spread
    )
    left = jnp.concatenate(inverse, axis=0)
    whole = jnp.concatenate(upper + [jnp.zeros((LANES - width, LANES), F32)], axis=0).T
    whole = jnp.where(r >= c, whole, 0.0)[:width, :width]
    lower_out[...] = whole * scale[...]
    chunks = sems.shape[0] - 1
    copies = [pltpu.make_async_copy(lower_out, factor, sems.at[chunks])]
    copies[0].start()
    w_high, w_low = split(left[:, :width])
    wm = jnp.concatenate([w_high[:, :modes], w_low[:, :modes]], axis=0)
    ws = jnp.concatenate([w_high[:, modes:], w_low[:, modes:]], axis=0)
    both_w = jnp.concatenate([wm, wm, ws, ws], axis=1)
    slabs = buf.shape[1]
    flat = buf.reshape(width * slabs, LANES)
    step = slabs // chunks
    for k in range(chunks):
        cols = slice(k * step * LANES, (k + 1) * step * LANES)
        right = jnp.concatenate([modes_panel[:, cols], snaps_panel[:, cols]], axis=0)
        res = jnp.dot(both_w, right, preferred_element_type=F32)
        res = res[:width] + res[width:]
        for i in range(step):
            flat[pl.ds(k * step + i, width, stride=slabs), :] = res[:, i * LANES:(i + 1) * LANES]
        part = (slice(None), pl.ds(k * step, step))
        copies.append(pltpu.make_async_copy(buf.at[part], out.at[part], sems.at[k]))
        copies[-1].start()
    for copy in copies:
        copy.wait()


def per_device(basis_modes, weights, snapshots):
    modes, rows, cols = basis_modes.shape
    snaps = snapshots.shape[0]
    width = modes + snaps
    tiles = cols // LANES
    slabs = rows * tiles
    cores = lax.axis_size("grp")
    cells = rows * cols * lax.axis_size("srv") * cores
    fields = basis_modes.reshape(modes, rows, tiles, LANES).transpose(0, 2, 1, 3)
    fields = fields.reshape(modes * slabs, LANES)
    own = snapshots.reshape(snaps, cores * rows, tiles // cores, LANES)
    own = with_layout_constraint(own, Layout((0, 2, 1, 3))).transpose(0, 2, 1, 3)
    own = own.reshape(snaps * tiles * rows, LANES)
    ones = pl.pallas_call(
        ones_kernel,
        out_shape=jax.ShapeDtypeStruct((1, snaps), F32),
        out_specs=VMEM,
        compiler_params=PARAMS,
        cost_estimate=pl.CostEstimate(flops=COST, bytes_accessed=10**6, transcendentals=0),
        name="ones_row",
    )()
    fields, ones = lax.optimization_barrier((fields, ones))
    got = lax.ppermute(own, "grp", [(0, 1), (1, 0)])

    chunk = 6
    modes_panel, modes_gram = pl.pallas_call(
        modes_kernel,
        out_shape=(
            jax.ShapeDtypeStruct((2 * modes, slabs * LANES), BF16),
            jax.ShapeDtypeStruct((2 * modes, modes), F32),
        ),
        in_specs=[VMEM],
        out_specs=(VMEM, VMEM),
        cost_estimate=pl.CostEstimate(flops=10**8, bytes_accessed=fields.size * 4, transcendentals=0),
        compiler_params=PARAMS,
        name="modes_gram",
    )(fields)
    snaps_panel, packed = pl.pallas_call(
        functools.partial(snaps_kernel, rows),
        out_shape=(
            jax.ShapeDtypeStruct((2 * snaps, slabs * LANES), BF16),
            jax.ShapeDtypeStruct((len(packing(width)) * BLOCK, LANES), F32),
        ),
        in_specs=[VMEM] * 4,
        out_specs=(VMEM, VMEM),
        compiler_params=PARAMS,
        cost_estimate=pl.CostEstimate(flops=10**8, bytes_accessed=10**6, transcendentals=0),
        name="snaps_gram",
    )(own, got, modes_panel, modes_gram)
    packed = total(packed)
    scale = jnp.concatenate([weights, ones[0]])
    new_modes, factor = pl.pallas_call(
        functools.partial(apply_kernel, cells),
        out_shape=(
            jax.ShapeDtypeStruct((width, slabs, LANES), F32),
            jax.ShapeDtypeStruct((width, width), F32),
        ),
        in_specs=[VMEM] * 4,
        out_specs=(ANY, ANY),
        scratch_shapes=[
            pltpu.VMEM((width, slabs, LANES), F32),
            pltpu.VMEM((width, width), F32),
            pltpu.SemaphoreType.DMA((chunk + 1,)),
            *(pltpu.VMEM((n, TILE * TILE, LANES), F32) for n in (width // TILE, 2, 2, width // TILE)),
        ],
        compiler_params=PARAMS,
        name="factor_apply",
    )(packed, scale[:, None], modes_panel, snaps_panel)
    new_modes = new_modes.reshape(width, tiles, rows, LANES).transpose(0, 2, 1, 3)
    return new_modes.reshape(width, rows, cols), factor


def solution(mesh):
    in_specs = (P(None, AXES, None), P(), P(None, "srv", "grp"))
    out_specs = (P(None, AXES, None), P())
    return jax.shard_map(
        per_device, mesh=mesh, in_specs=in_specs, out_specs=out_specs, check_vma=False
    )
```

```python
import functools
import jax
import jax.numpy as jnp
from jax import lax
from jax.experimental.layout import Layout, with_layout_constraint
from jax.experimental import pallas as pl
from jax.experimental.pallas import tpu as pltpu
from jax.sharding import PartitionSpec as P

AXES = ("srv", "grp")
LANES = 128
TILE = 8
BLOCK = 16
PIECES = 2
F32, BF16 = jnp.float32, jnp.bfloat16
VMEM = pl.BlockSpec(memory_space=pltpu.VMEM)
ANY = pl.BlockSpec(memory_space=pl.ANY)
HBM = pl.BlockSpec(memory_space=pltpu.HBM)
PARAMS = pltpu.CompilerParams(vmem_limit_bytes=16 * 2**20)


def total(value):
    servers, cores = lax.axis_size("srv"), lax.axis_size("grp")
    if servers & (servers - 1) or servers < 4 or cores != 2:
        return lax.psum(value, AXES)
    count = servers * cores
    masks = [2 << p | 1 for p in range(servers.bit_length() - 1)]
    rounds = [[1]] + [[mask] for mask in masks[3:]] + [[masks[0], masks[1], masks[0] | masks[1]]] + [[mask] for mask in masks[2:3]]
    for masks in rounds:
        parts = [lax.ppermute(value, AXES, [(i, i ^ m) for i in range(count)]) for m in masks]
        for part in parts:
            value = value + part
    return value


def packing(width):
    groups = []
    for r in reversed(range(width // BLOCK)):
        for group in groups:
            if sum(q + 1 for q in group) + r + 1 <= LANES // BLOCK:
                group.append(r)
                break
        else:
            groups.append([r])
    return groups


def split(x):
    high = x.astype(BF16)
    return high, (x - high.astype(F32)).astype(BF16)


def rows_times_rows(a, b):
    return lax.dot_general(a, b, (((1,), (1,)), ((), ())), preferred_element_type=F32)


def modes_kernel(source, panel, gram, buf, sems):
    count, slabs, _ = source.shape
    flat = buf.reshape(count * slabs, LANES)
    pieces = sems.shape[0]
    step = slabs // pieces
    copies = []
    for p in range(pieces):
        part = (slice(None), pl.ds(p * step, step))
        copies.append(pltpu.make_async_copy(source.at[part], buf.at[part], sems.at[p]))
        copies[-1].start()
    terms = []
    for p in range(pieces):
        copies[p].wait()
        for i in range(p * step, (p + 1) * step):
            high, low = split(flat[pl.ds(i, count, stride=slabs), :])
            panel[:count, i * LANES:(i + 1) * LANES] = high
            panel[count:, i * LANES:(i + 1) * LANES] = low
        cols = slice(p * step * LANES, (p + 1) * step * LANES)
        terms.append(rows_times_rows(panel[:, cols], panel[:count, cols]))
    gram[...] = total_of(terms)


def snaps_kernel(rows, keep, got, modes_panel, modes_gram, panel, packed):
    snaps, modes = panel.shape[0] // 2, modes_gram.shape[1]
    core = lax.axis_index("grp")
    stride = keep.shape[0] // snaps
    here = stride // 2
    for h in (0, 1):
        for i in range(here):
            start = i // rows * 2 * rows + core * rows + i % rows
            place = pl.ds(start, snaps, stride=stride)
            high, low = split(jnp.where(core == h, keep[place, :], got[place, :]))
            at = (h * here + i) * LANES
            panel[:snaps, at:at + LANES] = high
            panel[snaps:, at:at + LANES] = low
    high = jnp.concatenate([modes_panel[:modes], panel[:snaps]], axis=0)
    low = jnp.concatenate([modes_panel[modes:], panel[snaps:]], axis=0)
    both = rows_times_rows(panel[...], high)
    last = both[:snaps] + both[snaps:] + rows_times_rows(panel[:snaps], low)
    cross = modes_gram[modes:]
    whole = jnp.concatenate([modes_gram[:modes] + cross + cross.T, jnp.zeros((modes, snaps), F32)], axis=1)
    whole = jnp.concatenate([whole, last], axis=0)
    for g, group in enumerate(packing(modes + snaps)):
        parts = [whole[r * BLOCK:(r + 1) * BLOCK, :(r + 1) * BLOCK] for r in group]
        spare = LANES - sum(p.shape[1] for p in parts)
        if spare:
            parts.append(jnp.zeros((BLOCK, spare), F32))
        packed[g * BLOCK:(g + 1) * BLOCK, :] = jnp.concatenate(parts, axis=1)


def spread_row(x, i):
    return jnp.broadcast_to(x[i:i + 1, :], (TILE, LANES))


def spread_column(x, j):
    return jnp.broadcast_to(x[:, j:j + 1], (x.shape[0], LANES))


def total_of(terms):
    terms = list(terms)
    while len(terms) > 1:
        terms = [sum(terms[i:i + 2]) for i in range(0, len(terms), 2)]
    return terms[0]


def everywhere(ref, row):
    return jnp.broadcast_to(ref[row:row + 1, :], (TILE, LANES))


def block_inverse(a):
    a = dict(a)
    l, m = {}, {}
    for p in range(0, TILE, 2):
        q = p + 1
        root = lax.rsqrt(a[p, p])
        det = a[p, p] * a[q, q] - a[q, p] * a[q, p]
        root_det = lax.rsqrt(det)
        over_det = root_det * root_det
        m[p, p] = root
        m[q, q] = root_det * (a[p, p] * root)
        l[q, p] = a[q, p] * root
        both = root_det * root
        w, z = {}, {}
        for i in range(q + 1, TILE):
            w[i] = a[p, p] * a[i, q] - a[q, p] * a[i, p]
            z[i] = a[q, q] * a[i, p] - a[q, p] * a[i, q]
            l[i, p] = a[i, p] * root
            l[i, q] = w[i] * both
        for k in range(q + 1, TILE):
            for i in range(k, TILE):
                a[i, k] = a[i, k] - (a[i, p] * z[k] + a[i, q] * w[k]) * over_det
        for i in (p, q):
            for k in range(i):
                m[i, k] = -m[i, i] * total_of(l[i, j] * m[j, k] for j in range(k, i))
    return m


def factor_tiles(tiles, lower, entries, columns_of, rows_of, solved_of):
    count = len(tiles)
    lane = lax.broadcasted_iota(jnp.int32, (TILE, LANES), 1)
    tiles = list(tiles)
    upper, inverse = [], []
    square = TILE * TILE
    for b in range(2):
        columns_of[b] = jnp.zeros((square, LANES), F32)
        rows_of[b] = jnp.zeros((square, LANES), F32)
    diagonal = [spread_column(lower[0], j) for j in range(TILE)]
    below = [[spread_column(x, j) for j in range(TILE)] for x in lower[1:]]
    following = [spread_column(lower[1], TILE + j) for j in range(TILE)]
    for t in range(count):
        at = t * TILE
        slot = entries.at[t]
        for j in range(TILE):
            slot[j * TILE:(j + 1) * TILE, :] = diagonal[j]
        m = block_inverse(
            {(i, j): everywhere(slot, j * TILE + i) for j in range(TILE) for i in range(j, TILE)}
        )
        if t + 1 < count:
            ahead = solved_of.at[t]
            for i in range(TILE):
                solved = total_of(m[i, j] * below[0][j] for j in range(i + 1))
                ahead[i * TILE:(i + 1) * TILE, :] = solved
            kept = [ahead[i * TILE:(i + 1) * TILE, :] for i in range(TILE)]
            diagonal = [
                following[k]
                - total_of(kept[i] * everywhere(ahead, i * TILE + k) for i in range(TILE))
                for k in range(TILE)
            ]
        by_column, by_row = columns_of.at[t % 2], rows_of.at[t % 2]
        for i in range(TILE):
            for k in range(i + 1):
                by_column[k * TILE + i:k * TILE + i + 1, :] = m[i, k][:1]
                by_row[i * TILE + k:i * TILE + k + 1, :] = m[i, k][:1]
        m_columns = [by_column[k * TILE:(k + 1) * TILE, :] for k in range(TILE)]
        row = total_of(m_columns[k] * spread_row(tiles[t], k) for k in range(TILE))
        block = (lane >= at) & (lane < at + TILE)
        mixed = row
        for k in range(TILE):
            mixed = jnp.where(lane == at + k, m_columns[k], mixed)
        upper.append(row)
        inverse.append(jnp.where(lane < at + TILE, mixed, 0.0))
        if t + 1 == count:
            break
        solved = total_of(
            by_row[i * TILE:(i + 1) * TILE, :] * spread_row(mixed, i) for i in range(TILE)
        )
        rows = [spread_row(solved, j) for j in range(TILE)]
        for s in range(t + 1, count):
            c = below[s - t - 1]
            tiles[s] = jnp.where(block, 0.0, tiles[s]) - total_of(c[j] * rows[j] for j in range(TILE))
        below = [[spread_column(x, at + TILE + j) for j in range(TILE)] for x in tiles[t + 2:]]
        if t + 2 < count:
            following = [spread_column(tiles[t + 2], at + 2 * TILE + j) for j in range(TILE)]
    return upper, inverse


def apply_kernel(cells, packed, scale, modes_panel, snaps_panel, out, factor, buf, lower_out, sems, *spread):
    modes, snaps = modes_panel.shape[0] // 2, snaps_panel.shape[0] // 2
    width = modes + snaps
    lane = lax.broadcasted_iota(jnp.int32, (BLOCK, LANES), 1)
    parts = {}
    for g, group in enumerate(packing(width)):
        strip = packed[g * BLOCK:(g + 1) * BLOCK, :] * (1.0 / cells)
        used = 0
        for r in group:
            piece = pltpu.roll(strip, LANES - used, 1) if used else strip
            parts[r] = jnp.where(lane < (r + 1) * BLOCK, piece, 0.0)
            used += (r + 1) * BLOCK
    lower = [parts[r] for r in range(width // BLOCK)] + [jnp.zeros((LANES - width, LANES), F32)]
    lower = jnp.concatenate(lower, axis=0)
    r = lax.broadcasted_iota(jnp.int32, (LANES, LANES), 0)
    c = lax.broadcasted_iota(jnp.int32, (LANES, LANES), 1)
    full = jnp.where(r >= c, lower, lower.T)
    upper, inverse = factor_tiles(
        *([x[i:i + TILE] for i in range(0, width, TILE)] for x in (full, lower)), *spread
    )
    left = jnp.concatenate(inverse, axis=0)
    whole = jnp.concatenate(upper + [jnp.zeros((LANES - width, LANES), F32)], axis=0).T
    whole = jnp.where(r >= c, whole, 0.0)[:width, :width]
    lower_out[...] = whole * scale[...]
    chunks = sems.shape[0] - 1
    copies = [pltpu.make_async_copy(lower_out, factor, sems.at[chunks])]
    copies[0].start()
    w_high, w_low = split(left[:, :width])
    wm = jnp.concatenate([w_high[:, :modes], w_low[:, :modes]], axis=0)
    ws = jnp.concatenate([w_high[:, modes:], w_low[:, modes:]], axis=0)
    both_w = jnp.concatenate([wm, wm, ws, ws], axis=1)
    slabs = buf.shape[1]
    flat = buf.reshape(width * slabs, LANES)
    step = slabs // chunks

    def product(k):
        cols = slice(k * step * LANES, (k + 1) * step * LANES)
        right = jnp.concatenate([modes_panel[:, cols], snaps_panel[:, cols]], axis=0)
        res = jnp.dot(both_w, right, preferred_element_type=F32)
        return res[:width] + res[width:]

    following = product(0)
    for k in range(chunks):
        res = following
        if k + 1 < chunks:
            following = product(k + 1)
        for i in range(step):
            flat[pl.ds(k * step + i, width, stride=slabs), :] = res[:, i * LANES:(i + 1) * LANES]
        part = (slice(None), pl.ds(k * step, step))
        copies.append(pltpu.make_async_copy(buf.at[part], out.at[part], sems.at[k]))
        copies[-1].start()
    for copy in copies:
        copy.wait()


def per_device(basis_modes, weights, snapshots):
    modes, rows, cols = basis_modes.shape
    snaps = snapshots.shape[0]
    width = modes + snaps
    tiles = cols // LANES
    slabs = rows * tiles
    cores = lax.axis_size("grp")
    cells = rows * cols * lax.axis_size("srv") * cores
    fields = basis_modes.reshape(modes, rows, tiles, LANES).transpose(0, 2, 1, 3)
    fields = pltpu.with_memory_space_constraint(fields.reshape(modes, slabs, LANES), pltpu.HBM)
    own = snapshots.reshape(snaps, cores * rows, tiles // cores, LANES)
    own = with_layout_constraint(own, Layout((0, 2, 1, 3))).transpose(0, 2, 1, 3)
    own = own.reshape(snaps * tiles * rows, LANES)
    got = lax.ppermute(own, "grp", [(0, 1), (1, 0)])

    chunk = 12
    modes_panel, modes_gram = pl.pallas_call(
        modes_kernel,
        out_shape=(
            jax.ShapeDtypeStruct((2 * modes, slabs * LANES), BF16),
            jax.ShapeDtypeStruct((2 * modes, modes), F32),
        ),
        in_specs=[HBM],
        out_specs=(VMEM, VMEM),
        scratch_shapes=[pltpu.VMEM(fields.shape, F32), pltpu.SemaphoreType.DMA((PIECES,))],
        cost_estimate=pl.CostEstimate(flops=10**8, bytes_accessed=fields.size * 4, transcendentals=0),
        compiler_params=PARAMS,
        name="modes_gram",
    )(fields)
    snaps_panel, packed = pl.pallas_call(
        functools.partial(snaps_kernel, rows),
        out_shape=(
            jax.ShapeDtypeStruct((2 * snaps, slabs * LANES), BF16),
            jax.ShapeDtypeStruct((len(packing(width)) * BLOCK, LANES), F32),
        ),
        in_specs=[VMEM] * 4,
        out_specs=(VMEM, VMEM),
        compiler_params=PARAMS,
        cost_estimate=pl.CostEstimate(flops=10**8, bytes_accessed=10**6, transcendentals=0),
        name="snaps_gram",
    )(own, got, modes_panel, modes_gram)
    packed = total(packed)
    scale = jnp.concatenate([weights, jnp.ones((snaps,), F32)])
    new_modes, factor = pl.pallas_call(
        functools.partial(apply_kernel, cells),
        out_shape=(
            jax.ShapeDtypeStruct((width, slabs, LANES), F32),
            jax.ShapeDtypeStruct((width, width), F32),
        ),
        in_specs=[VMEM] * 4,
        out_specs=(ANY, ANY),
        scratch_shapes=[
            pltpu.VMEM((width, slabs, LANES), F32),
            pltpu.VMEM((width, width), F32),
            pltpu.SemaphoreType.DMA((chunk + 1,)),
            *(pltpu.VMEM((n, TILE * TILE, LANES), F32) for n in (width // TILE, 2, 2, width // TILE)),
        ],
        compiler_params=PARAMS,
        name="factor_apply",
    )(packed, scale[:, None], modes_panel, snaps_panel)
    new_modes = new_modes.reshape(width, tiles, rows, LANES).transpose(0, 2, 1, 3)
    return new_modes.reshape(width, rows, cols), factor


def solution(mesh):
    in_specs = (P(None, AXES, None), P(), P(None, "srv", "grp"))
    out_specs = (P(None, AXES, None), P())
    return jax.shard_map(
        per_device, mesh=mesh, in_specs=in_specs, out_specs=out_specs, check_vma=False
    )
```

```python
import functools
import jax
import jax.numpy as jnp
from jax import lax
from jax.experimental.layout import Layout, with_layout_constraint
from jax.experimental import pallas as pl
from jax.experimental.pallas import tpu as pltpu
from jax.sharding import PartitionSpec as P

AXES = ("srv", "grp")
LANES = 128
TILE = 8
BLOCK = 16
PIECES = 2
F32, BF16 = jnp.float32, jnp.bfloat16
VMEM = pl.BlockSpec(memory_space=pltpu.VMEM)
ANY = pl.BlockSpec(memory_space=pl.ANY)
HBM = pl.BlockSpec(memory_space=pltpu.HBM)
PARAMS = pltpu.CompilerParams(vmem_limit_bytes=16 * 2**20)


def total(value):
    servers, cores = lax.axis_size("srv"), lax.axis_size("grp")
    if servers & (servers - 1) or servers < 4 or cores != 2:
        return lax.psum(value, AXES)
    count = servers * cores
    masks = [2 << p | 1 for p in range(servers.bit_length() - 1)]
    rounds = [[1]] + [[mask] for mask in masks[3:]] + [[masks[0], masks[1], masks[0] | masks[1]]] + [[mask] for mask in masks[2:3]]
    for masks in rounds:
        parts = [lax.ppermute(value, AXES, [(i, i ^ m) for i in range(count)]) for m in masks]
        for part in parts:
            value = value + part
    return value


def packing(width):
    groups = []
    for r in reversed(range(width // BLOCK)):
        for group in groups:
            if sum(q + 1 for q in group) + r + 1 <= LANES // BLOCK:
                group.append(r)
                break
        else:
            groups.append([r])
    return groups


def split(x):
    high = x.astype(BF16)
    return high, (x - high.astype(F32)).astype(BF16)


def rows_times_rows(a, b):
    return lax.dot_general(a, b, (((1,), (1,)), ((), ())), preferred_element_type=F32)


def modes_kernel(source, panel, gram, buf, sems):
    count, slabs, _ = source.shape
    flat = buf.reshape(count * slabs, LANES)
    pieces = sems.shape[0]
    step = slabs // pieces
    copies = []
    for p in range(pieces):
        part = (slice(None), pl.ds(p * step, step))
        copies.append(pltpu.make_async_copy(source.at[part], buf.at[part], sems.at[p]))
        copies[-1].start()
    terms = []
    for p in range(pieces):
        copies[p].wait()
        for i in range(p * step, (p + 1) * step):
            high, low = split(flat[pl.ds(i, count, stride=slabs), :])
            panel[:count, i * LANES:(i + 1) * LANES] = high
            panel[count:, i * LANES:(i + 1) * LANES] = low
        cols = slice(p * step * LANES, (p + 1) * step * LANES)
        terms.append(rows_times_rows(panel[:, cols], panel[:count, cols]))
    gram[...] = total_of(terms)


def snaps_kernel(rows, keep, got, modes_panel, modes_gram, panel, packed):
    snaps, modes = panel.shape[0] // 2, modes_gram.shape[1]
    core = lax.axis_index("grp")
    stride = keep.shape[0] // snaps
    here = stride // 2
    for h in (0, 1):
        for i in range(here):
            start = i // rows * 2 * rows + core * rows + i % rows
            place = pl.ds(start, snaps, stride=stride)
            high, low = split(jnp.where(core == h, keep[place, :], got[place, :]))
            at = (h * here + i) * LANES
            panel[:snaps, at:at + LANES] = high
            panel[snaps:, at:at + LANES] = low
    high = jnp.concatenate([modes_panel[:modes], panel[:snaps]], axis=0)
    low = jnp.concatenate([modes_panel[modes:], panel[snaps:]], axis=0)
    both = rows_times_rows(panel[...], high)
    last = both[:snaps] + both[snaps:] + rows_times_rows(panel[:snaps], low)
    cross = modes_gram[modes:]
    whole = jnp.concatenate([modes_gram[:modes] + cross + cross.T, jnp.zeros((modes, snaps), F32)], axis=1)
    whole = jnp.concatenate([whole, last], axis=0)
    for g, group in enumerate(packing(modes + snaps)):
        parts = [whole[r * BLOCK:(r + 1) * BLOCK, :(r + 1) * BLOCK] for r in group]
        spare = LANES - sum(p.shape[1] for p in parts)
        if spare:
            parts.append(jnp.zeros((BLOCK, spare), F32))
        packed[g * BLOCK:(g + 1) * BLOCK, :] = jnp.concatenate(parts, axis=1)


def spread_row(x, i):
    return jnp.broadcast_to(x[i:i + 1, :], (TILE, LANES))


def spread_column(x, j):
    return jnp.broadcast_to(x[:, j:j + 1], (x.shape[0], LANES))


def total_of(terms):
    terms = list(terms)
    while len(terms) > 1:
        terms = [sum(terms[i:i + 2]) for i in range(0, len(terms), 2)]
    return terms[0]


def everywhere(ref, row):
    return jnp.broadcast_to(ref[row:row + 1, :], (TILE, LANES))


def block_inverse(a):
    a = dict(a)
    l, m = {}, {}
    for p in range(0, TILE, 2):
        q = p + 1
        root = lax.rsqrt(a[p, p])
        det = a[p, p] * a[q, q] - a[q, p] * a[q, p]
        root_det = lax.rsqrt(det)
        over_det = root_det * root_det
        m[p, p] = root
        m[q, q] = root_det * (a[p, p] * root)
        l[q, p] = a[q, p] * root
        both = root_det * root
        w, z = {}, {}
        for i in range(q + 1, TILE):
            w[i] = a[p, p] * a[i, q] - a[q, p] * a[i, p]
            z[i] = a[q, q] * a[i, p] - a[q, p] * a[i, q]
            l[i, p] = a[i, p] * root
            l[i, q] = w[i] * both
        for k in range(q + 1, TILE):
            for i in range(k, TILE):
                a[i, k] = a[i, k] - (a[i, p] * z[k] + a[i, q] * w[k]) * over_det
        for i in (p, q):
            for k in range(i):
                m[i, k] = -m[i, i] * total_of(l[i, j] * m[j, k] for j in range(k, i))
    return m


def factor_tiles(tiles, lower, entries, columns_of, rows_of, solved_of):
    count = len(tiles)
    lane = lax.broadcasted_iota(jnp.int32, (TILE, LANES), 1)
    tiles = list(tiles)
    upper, inverse = [], []
    square = TILE * TILE
    for b in range(2):
        columns_of[b] = jnp.zeros((square, LANES), F32)
        rows_of[b] = jnp.zeros((square, LANES), F32)
    diagonal = [spread_column(lower[0], j) for j in range(TILE)]
    below = [[spread_column(x, j) for j in range(TILE)] for x in lower[1:]]
    following = [spread_column(lower[1], TILE + j) for j in range(TILE)]
    for t in range(count):
        at = t * TILE
        slot = entries.at[t]
        for j in range(TILE):
            slot[j * TILE:(j + 1) * TILE, :] = diagonal[j]
        m = block_inverse(
            {(i, j): everywhere(slot, j * TILE + i) for j in range(TILE) for i in range(j, TILE)}
        )
        if t + 1 < count:
            ahead = solved_of.at[t]
            for i in range(TILE):
                solved = total_of(m[i, j] * below[0][j] for j in range(i + 1))
                ahead[i * TILE:(i + 1) * TILE, :] = solved
            kept = [ahead[i * TILE:(i + 1) * TILE, :] for i in range(TILE)]
            diagonal = [
                following[k]
                - total_of(kept[i] * everywhere(ahead, i * TILE + k) for i in range(TILE))
                for k in range(TILE)
            ]
        by_column, by_row = columns_of.at[t % 2], rows_of.at[t % 2]
        for i in range(TILE):
            for k in range(i + 1):
                by_column[k * TILE + i:k * TILE + i + 1, :] = m[i, k][:1]
                by_row[i * TILE + k:i * TILE + k + 1, :] = m[i, k][:1]
        m_columns = [by_column[k * TILE:(k + 1) * TILE, :] for k in range(TILE)]
        row = total_of(m_columns[k] * spread_row(tiles[t], k) for k in range(TILE))
        block = (lane >= at) & (lane < at + TILE)
        mixed = row
        for k in range(TILE):
            mixed = jnp.where(lane == at + k, m_columns[k], mixed)
        upper.append(row)
        inverse.append(jnp.where(lane < at + TILE, mixed, 0.0))
        if t + 1 == count:
            break
        solved = total_of(
            by_row[i * TILE:(i + 1) * TILE, :] * spread_row(mixed, i) for i in range(TILE)
        )
        rows = [spread_row(solved, j) for j in range(TILE)]
        for s in range(t + 1, count):
            c = below[s - t - 1]
            tiles[s] = jnp.where(block, 0.0, tiles[s]) - total_of(c[j] * rows[j] for j in range(TILE))
        below = [[spread_column(x, at + TILE + j) for j in range(TILE)] for x in tiles[t + 2:]]
        if t + 2 < count:
            following = [spread_column(tiles[t + 2], at + 2 * TILE + j) for j in range(TILE)]
    return upper, inverse


def apply_kernel(cells, packed, scale, modes_panel, snaps_panel, out, factor, buf, lower_out, sems, *spread):
    modes, snaps = modes_panel.shape[0] // 2, snaps_panel.shape[0] // 2
    width = modes + snaps
    lane = lax.broadcasted_iota(jnp.int32, (BLOCK, LANES), 1)
    parts = {}
    for g, group in enumerate(packing(width)):
        strip = packed[g * BLOCK:(g + 1) * BLOCK, :] * (1.0 / cells)
        used = 0
        for r in group:
            piece = pltpu.roll(strip, LANES - used, 1) if used else strip
            parts[r] = jnp.where(lane < (r + 1) * BLOCK, piece, 0.0)
            used += (r + 1) * BLOCK
    lower = [parts[r] for r in range(width // BLOCK)] + [jnp.zeros((LANES - width, LANES), F32)]
    lower = jnp.concatenate(lower, axis=0)
    r = lax.broadcasted_iota(jnp.int32, (LANES, LANES), 0)
    c = lax.broadcasted_iota(jnp.int32, (LANES, LANES), 1)
    full = jnp.where(r >= c, lower, lower.T)
    upper, inverse = factor_tiles(
        *([x[i:i + TILE] for i in range(0, width, TILE)] for x in (full, lower)), *spread
    )
    left = jnp.concatenate(inverse, axis=0)
    whole = jnp.concatenate(upper + [jnp.zeros((LANES - width, LANES), F32)], axis=0).T
    whole = jnp.where(r >= c, whole, 0.0)[:width, :width]
    lower_out[...] = whole * scale[...]
    chunks = sems.shape[0] - 1
    copies = [pltpu.make_async_copy(lower_out, factor, sems.at[chunks])]
    copies[0].start()
    w_high, w_low = split(left[:, :width])
    wm = jnp.concatenate([w_high[:, :modes], w_low[:, :modes]], axis=0)
    ws = jnp.concatenate([w_high[:, modes:], w_low[:, modes:]], axis=0)
    both_w = jnp.concatenate([wm, wm, ws, ws], axis=1)
    slabs = buf.shape[1]
    flat = buf.reshape(width * slabs, LANES)
    step = slabs // chunks

    def product(k):
        cols = slice(k * step * LANES, (k + 1) * step * LANES)
        right = jnp.concatenate([modes_panel[:, cols], snaps_panel[:, cols]], axis=0)
        res = jnp.dot(both_w, right, preferred_element_type=F32)
        return res[:width] + res[width:]

    following = product(0)
    for k in range(chunks):
        res = following
        if k + 1 < chunks:
            following = product(k + 1)
        for i in range(step):
            flat[pl.ds(k * step + i, width, stride=slabs), :] = res[:, i * LANES:(i + 1) * LANES]
        part = (slice(None), pl.ds(k * step, step))
        copies.append(pltpu.make_async_copy(buf.at[part], out.at[part], sems.at[k]))
        copies[-1].start()
    for copy in copies:
        copy.wait()


def per_device(basis_modes, weights, snapshots):
    modes, rows, cols = basis_modes.shape
    snaps = snapshots.shape[0]
    width = modes + snaps
    tiles = cols // LANES
    slabs = rows * tiles
    cores = lax.axis_size("grp")
    cells = rows * cols * lax.axis_size("srv") * cores
    fields = basis_modes.reshape(modes, rows, tiles, LANES).transpose(0, 2, 1, 3)
    fields = pltpu.with_memory_space_constraint(fields.reshape(modes, slabs, LANES), pltpu.HBM)
    own = snapshots.reshape(snaps, cores * rows, tiles // cores, LANES)
    own = with_layout_constraint(own, Layout((0, 2, 1, 3))).transpose(0, 2, 1, 3)
    own = own.reshape(snaps * tiles * rows, LANES)
    got = lax.ppermute(own, "grp", [(0, 1), (1, 0)])

    chunk = 6
    modes_panel, modes_gram = pl.pallas_call(
        modes_kernel,
        out_shape=(
            jax.ShapeDtypeStruct((2 * modes, slabs * LANES), BF16),
            jax.ShapeDtypeStruct((2 * modes, modes), F32),
        ),
        in_specs=[HBM],
        out_specs=(VMEM, VMEM),
        scratch_shapes=[pltpu.VMEM(fields.shape, F32), pltpu.SemaphoreType.DMA((PIECES,))],
        cost_estimate=pl.CostEstimate(flops=10**8, bytes_accessed=fields.size * 4, transcendentals=0),
        compiler_params=PARAMS,
        name="modes_gram",
    )(fields)
    snaps_panel, packed = pl.pallas_call(
        functools.partial(snaps_kernel, rows),
        out_shape=(
            jax.ShapeDtypeStruct((2 * snaps, slabs * LANES), BF16),
            jax.ShapeDtypeStruct((len(packing(width)) * BLOCK, LANES), F32),
        ),
        in_specs=[VMEM] * 4,
        out_specs=(VMEM, VMEM),
        compiler_params=PARAMS,
        cost_estimate=pl.CostEstimate(flops=10**8, bytes_accessed=10**6, transcendentals=0),
        name="snaps_gram",
    )(own, got, modes_panel, modes_gram)
    packed = total(packed)
    scale = jnp.concatenate([weights, jnp.ones((snaps,), F32)])
    new_modes, factor = pl.pallas_call(
        functools.partial(apply_kernel, cells),
        out_shape=(
            jax.ShapeDtypeStruct((width, slabs, LANES), F32),
            jax.ShapeDtypeStruct((width, width), F32),
        ),
        in_specs=[VMEM] * 4,
        out_specs=(ANY, ANY),
        scratch_shapes=[
            pltpu.VMEM((width, slabs, LANES), F32),
            pltpu.VMEM((width, width), F32),
            pltpu.SemaphoreType.DMA((chunk + 1,)),
            *(pltpu.VMEM((n, TILE * TILE, LANES), F32) for n in (width // TILE, 2, 2, width // TILE)),
        ],
        compiler_params=PARAMS,
        name="factor_apply",
    )(packed, scale[:, None], modes_panel, snaps_panel)
    new_modes = new_modes.reshape(width, tiles, rows, LANES).transpose(0, 2, 1, 3)
    return new_modes.reshape(width, rows, cols), factor


def solution(mesh):
    in_specs = (P(None, AXES, None), P(), P(None, "srv", "grp"))
    out_specs = (P(None, AXES, None), P())
    return jax.shard_map(
        per_device, mesh=mesh, in_specs=in_specs, out_specs=out_specs, check_vma=False
    )
```
